256 devices in a mesh: group: 32 (over x, z), member: 8 (over y, core).
Axes of the slice: x: 4, y: 4, z: 8, core: 2. Of those that a mesh axis runs over, the one named last changes fastest.
Arguments:
- particles: float32 [8, 524288], P(None, ('group', 'member')), may hold values from 0 to 20, as said below
- new_slot: int32 [4096], P(('group', 'member')), may hold values from 0 to 4095, as said below
- neighbours: int32 [4096, 6], P(('group', 'member')), may hold values from 0 to 23, as said below
- ghosts: int32 [256, 2], P(('group', 'member')), may hold values from 0 to 4, as said below
Outputs:
- energy: float32 [524288], P(('group', 'member'))
- density: float32 [524288], P(('group', 'member'))
The draws below stay inside these ranges and needn't reach their ends.
Inputs may be any that keep to these rules, and one draw needn't show every extreme that they name: A permutation of 0 to 4095. Tile t goes to segment new_slot[t] // 16, where segment number = group index * 8 + member index; a tile keeps its member index. Every segment receives 16 tiles, no segment sends more than 2 tiles to one segment, and some segment sends exactly 2 tiles to one segment. `ghosts`: row d holds the number of tiles that segment d takes from the end of segment d - 1 and from the start of segment d + 1. Both are at least 1 except the first segment's left count and the last segment's right count, which are 0; some segment takes exactly 4 tiles from its left neighbour. `neighbours`: for moved tile s of segment d, entries count along the extended range: the last ghosts[d, 0] tiles of segment d - 1, then the 16 tiles of segment d, then the first ghosts[d, 1] tiles of segment d + 1; every entry lies inside that range, entry 0 is the tile itself, and entries may repeat. `particles`: Rows: positions within 0 to 1, masses within 0.5 / 768 to 2 / 768, smoothing lengths within 0.3 to 0.5, initial energies within 0.5 to 4, opacities within 0.05 to 20, heating within 0 to 1.
All inputs are finite; a program needn't handle non-finite values.
Results may differ from the reference program's by a relative error of at most 0.00014.
Values sent between devices are 32-bit elements; how exact they have to be, the bound alone decides.
No kernel may reach another device: no remote copies, remote signals or barrier semaphores. Data moves between devices by JAX's collectives and lax.ppermute only.
A program may use at most 64 MiB of HBM per device.

```python
import math
import jax
import jax.numpy as jnp
from jax import lax

TILE = 128
TD = 16
NB = 6
GMAX = 4
SWEEPS = 3
CAP = 2
GROUPS = 32
MEMBERS = 8
NTILES = 4096
NP = 524288
DEVICES = 256


def draw_particles(key, part):
    subkeys = jax.random.split(jax.random.fold_in(key, 11), 6)
    uniform_draw = jax.random.uniform(subkeys[0], (3, NP), jnp.float32)
    positions = uniform_draw
    masses = jnp.exp(jax.random.uniform(subkeys[1], (1, NP), jnp.float32, math.log(0.5), math.log(2.0))) / (NB * TILE)
    smooth = jax.random.uniform(subkeys[2], (1, NP), jnp.float32, 0.3, 0.5)
    energies = jnp.exp(jax.random.uniform(subkeys[3], (1, NP), jnp.float32, math.log(0.5), math.log(4.0)))
    opacity = jnp.exp(jax.random.uniform(subkeys[4], (1, NP), jnp.float32, math.log(0.05), math.log(20.0)))
    heating = jax.random.uniform(subkeys[5], (1, NP), jnp.float32, 0.0, 1.0)
    return jnp.concatenate([positions, masses, smooth, energies, opacity, heating], axis=0)


def ghost_table(key):
    base_key = jax.random.fold_in(key, 101)
    left_counts = jax.random.randint(jax.random.fold_in(base_key, 1), (DEVICES,), 1, GMAX + 1)
    right_counts = jax.random.randint(jax.random.fold_in(base_key, 2), (DEVICES,), 1, GMAX + 1)
    chosen = jax.random.randint(jax.random.fold_in(base_key, 3), (), 1, DEVICES)
    dev_ids = jnp.arange(DEVICES, dtype=jnp.int32)
    left_counts = jnp.where(dev_ids == chosen, GMAX, left_counts)
    left_counts = jnp.where(dev_ids == 0, 0, left_counts)
    right_counts = jnp.where(dev_ids == DEVICES - 1, 0, right_counts)
    return jnp.stack([left_counts, right_counts], axis=1).astype(jnp.int32)


def draw_ghosts(key, part):
    return ghost_table(key)


def draw_neighbours(key, part):
    table = ghost_table(key)
    tile_ids = jnp.arange(NTILES, dtype=jnp.int32)
    owner_dev = tile_ids // TD
    left_counts = table[owner_dev, 0]
    range_size = left_counts + TD + table[owner_dev, 1]
    itself = left_counts + tile_ids % TD
    others = jax.random.randint(jax.random.fold_in(key, 202), (NTILES, NB - 1), 0, range_size[:, None])
    return jnp.concatenate([itself[:, None], others], axis=1).astype(jnp.int32)


def member_counts(member_key):
    first_key, second_key = jax.random.split(member_key)
    unit_count = GROUPS * CAP
    specials = jnp.array([1 % GROUPS, GROUPS // 2 % GROUPS, (GROUPS - 1) % GROUPS], dtype=jnp.int32)
    keeper = specials[jax.random.randint(first_key, (), 0, 3)]
    unit_ids = jnp.arange(unit_count, dtype=jnp.int32)
    owners = unit_ids // CAP
    is_special = jnp.sum((owners[:, None] == specials[None, :]).astype(jnp.int32), axis=1) > 0
    first_unit = unit_ids % CAP == 0
    boost = jnp.where(owners == keeper, 3 * unit_count, 0) + jnp.where(is_special & first_unit, 2 * unit_count, 0)
    scores = jax.random.permutation(second_key, unit_count).astype(jnp.int32) + boost.astype(jnp.int32)
    ranked = jnp.argsort(-scores, stable=True)
    kept_units = jnp.zeros((unit_count,), jnp.int32).at[ranked[:TD]].set(1)
    return jnp.sum(kept_units.reshape(GROUPS, CAP), axis=1)


def order_of(order_key):
    return jax.random.permutation(order_key, TD).astype(jnp.int32)


def draw_new_slot(key, part):
    base_key = jax.random.fold_in(key, 303)
    counts = jax.vmap(member_counts)(jax.random.split(jax.random.fold_in(base_key, 1), MEMBERS))
    ends = jnp.cumsum(counts, axis=1)
    sender_order = jax.vmap(order_of)(jax.random.split(jax.random.fold_in(base_key, 2), DEVICES))
    receiver_order = jax.vmap(order_of)(jax.random.split(jax.random.fold_in(base_key, 3), DEVICES))
    tile_ids = jnp.arange(NTILES, dtype=jnp.int32)
    owner_dev = tile_ids // TD
    group_of = owner_dev // MEMBERS
    member_of = owner_dev % MEMBERS
    position = sender_order.reshape(-1)
    offset = jnp.sum((ends[member_of] <= position[:, None]).astype(jnp.int32), axis=1)
    dest_group = (group_of + offset) % GROUPS
    dest_dev = dest_group * MEMBERS + member_of
    new_slots = dest_dev * TD + receiver_order[dest_dev, position]
    return new_slots.astype(jnp.int32)


def setup_inputs(seed: int = 0) -> dict:
    key_list = jax.random.split(jax.random.key(seed), 5)
    return {
        "particles": draw_particles(jax.random.fold_in(key_list[4], 71), 0),
        "new_slot": draw_new_slot(jax.random.fold_in(key_list[4], 71), 0),
        "neighbours": draw_neighbours(jax.random.fold_in(key_list[4], 71), 0),
        "ghosts": draw_ghosts(jax.random.fold_in(key_list[4], 71), 0),
    }


KERNEL_NORM = 21.0 / (16.0 * math.pi)
TIME_STEP = 0.05

def geometry(own_fields, near_fields):
    offsets = near_fields[0:3, :, :, None, :] - own_fields[0:3, :, None, :, None]
    distance = jnp.sqrt(lax.optimization_barrier(jnp.sum(offsets * offsets, axis=0)))
    return (offsets, distance)

def pair_forces(own_fields, near_fields, distance):
    mean_smooth = 0.5 * (own_fields[4][:, None, :, None] + near_fields[4][:, :, None, :])
    falloff = jax.nn.relu(1.0 - 0.5 * distance / mean_smooth)
    return 5.0 * KERNEL_NORM * falloff ** 3 / mean_smooth ** 5

def density_kernel(own_items, near_items):
    own_fields = own_items[0]
    near_fields = near_items[0]
    offsets, distance = geometry(own_fields, near_fields)
    smooth = own_fields[4][:, None, :, None]
    scaled = distance / smooth
    falloff = jax.nn.relu(1.0 - 0.5 * scaled)
    weight = KERNEL_NORM * falloff ** 4 * (2.0 * scaled + 1.0) / smooth ** 3
    return lax.optimization_barrier(jnp.sum(near_fields[3][:, :, None, :] * weight, axis=(1, 3)))

def limiter_kernel(own_items, near_items):
    own_fields, own_density, own_energy = own_items
    near_fields, near_density, near_energy = near_items
    offsets, distance = geometry(own_fields, near_fields)
    forces = pair_forces(own_fields, near_fields, distance)
    volume = near_fields[3] / near_density[0]
    change = near_energy[0][:, :, None, :] - own_energy[0][:, None, :, None]
    scaled = volume[:, :, None, :] * forces * change
    gradient = lax.optimization_barrier(jnp.sum(scaled[None] * offsets, axis=(2, 4)))
    stream_ratio = jnp.sqrt(lax.optimization_barrier(jnp.sum(gradient * gradient, axis=0))) / (own_fields[6] * own_density[0] * own_energy[0])
    limiter = (2.0 + stream_ratio) / (6.0 + 3.0 * stream_ratio + stream_ratio * stream_ratio)
    return limiter / (own_fields[6] * own_density[0])

def jacobi_kernel(own_items, near_items):
    own_fields, own_density, own_diffusion = own_items
    near_fields, near_density, near_diffusion, near_energy = near_items
    offsets, distance = geometry(own_fields, near_fields)
    forces = pair_forces(own_fields, near_fields, distance)
    coupling = near_fields[3][:, :, None, :] * (own_diffusion[0][:, None, :, None] + near_diffusion[0][:, :, None, :]) * forces
    coupling = coupling / (own_density[0][:, None, :, None] * near_density[0][:, :, None, :])
    rate_sum = lax.optimization_barrier(jnp.sum(coupling, axis=(1, 3)))
    inflow = lax.optimization_barrier(jnp.sum(coupling * near_energy[0][:, :, None, :], axis=(1, 3)))
    return (own_fields[5] + TIME_STEP * own_fields[7] + TIME_STEP * inflow) / (1.0 + TIME_STEP * rate_sum)

def per_segment(kernel, own_items, all_items, near_index):

    def one_block(dev_id):
        first_tile = dev_id * TD
        own_part = tuple((lax.dynamic_slice_in_dim(values, first_tile, TD, 1) for values in own_items))
        near_rows = lax.dynamic_slice_in_dim(near_index, first_tile, TD, 0)
        near_part = tuple((jnp.take(values, near_rows, axis=1) for values in all_items))
        return kernel(own_part, near_part)
    blocks = lax.map(one_block, jnp.arange(DEVICES, dtype=jnp.int32))
    return blocks.reshape(1, NTILES, TILE)

def reference(particles, new_slot, neighbours, ghosts):
    tiled = particles.reshape(8, NTILES, TILE)
    arranged = jnp.zeros_like(tiled).at[:, new_slot, :].set(tiled)
    device = jnp.arange(NTILES, dtype=jnp.int32) // TD
    near_index = (device * TD - ghosts[device, 0])[:, None] + neighbours
    statics = arranged[0:6]
    density = per_segment(density_kernel, (arranged,), (statics,), near_index)
    energy = arranged[5:6]
    for sweep_step in range(SWEEPS):
        diffusion = per_segment(limiter_kernel, (arranged, density, energy), (statics, density, energy), near_index)
        energy = per_segment(jacobi_kernel, (arranged, density, diffusion), (statics, density, diffusion, energy), near_index)
    return (energy.reshape(-1), density.reshape(-1))
```

```python
import math

import jax
import jax.numpy as jnp
from jax import lax
from jax.experimental import pallas as pl
from jax.experimental.pallas import tpu as pltpu
from jax.sharding import PartitionSpec as P

TILE = 128
GMAX = 4
SWEEPS = 3
NB = 6
TD = 16
EXT = TD + 2 * GMAX
ROWS = 24
CHUNK = 32
KERNEL_NORM = 21.0 / (16.0 * math.pi)
TIME_STEP = 0.05
F32 = jnp.float32
BF16 = jnp.bfloat16
VMEM = pltpu.MemorySpace.VMEM
SMEM = pltpu.MemorySpace.SMEM
AXES = ("group", "member")


def call(body, outs, scratch, name, *args):
    specs = [
        pl.BlockSpec(memory_space=SMEM if a.dtype == jnp.int32 else VMEM) for a in args
    ]
    return pl.pallas_call(
        body,
        out_shape=[jax.ShapeDtypeStruct(shape, dtype) for shape, dtype in outs],
        in_specs=specs,
        out_specs=[pl.BlockSpec(memory_space=VMEM) for _ in outs],
        scratch_shapes=scratch,
        name=name,
        compiler_params=pltpu.CompilerParams(vmem_limit_bytes=40 * 1024 * 1024),
    )(*args)


def pack_body(slot, part, out, count):
    groups = out.shape[0]
    for g in range(groups):
        count[g] = 0
        out[g, 0:16] = jnp.zeros((16, TILE), F32)
        out[g, 16:24] = jnp.full((8, TILE), -1.0, F32)
    for t in range(TD):
        s = slot[t]
        g = s // (TD * 8)
        n = count[g]
        count[g] = n + 1
        out[g, pl.ds(pl.multiple_of(n * 8, 8), 8), :] = part[:, t * TILE : (t + 1) * TILE]
        out[g, pl.ds(16 + n, 1), :] = jnp.full((1, TILE), (s % TD).astype(F32))


def split3(x):
    hi = x.astype(BF16).astype(F32)
    rest = x - hi
    mid = rest.astype(BF16).astype(F32)
    return hi, mid, rest - mid


def send_parts(odd, values, first, second):
    n = values.shape[-2]
    tail = values[..., n - GMAX :, :]
    head = values[..., :GMAX, :]
    first[...] = jnp.where(odd, tail, head)
    second[...] = jnp.where(odd, head, tail)


def extend(odd, values, first, second):
    left = jnp.where(odd, second, first)
    right = jnp.where(odd, first, second)
    return jnp.concatenate([values, left, right], axis=-2)


def unpack_body(par, got, arranged, first, second):
    groups = got.shape[0] // ROWS
    odd = par[0] == 1
    lane = lax.broadcasted_iota(jnp.int32, (groups, TILE), 1).astype(F32)
    marks = [
        jnp.where(got[pl.ds(16 + n, groups, stride=ROWS), :] == lane, 1.0, 0.0) for n in range(2)
    ]
    marks.append(jnp.zeros((TILE - 2 * groups, TILE), F32))
    choose = jnp.concatenate(marks, axis=0).T[:TD, : 2 * groups].astype(BF16)
    for r in range(8):
        tiles = jnp.concatenate(
            [got[pl.ds(n * 8 + r, groups, stride=ROWS), :] for n in range(2)], axis=0
        )
        moved = sum(
            jnp.dot(choose, piece.astype(BF16), preferred_element_type=F32)
            for piece in split3(tiles)
        )
        arranged[r] = moved
    send_parts(odd, arranged[0:6], first, second)


def place_of(entry, left):
    j = entry - left
    return jnp.where(j < 0, j + TD + GMAX, jnp.where(j < TD, j, j + GMAX))


def pairs_body(par, near, ghosts, arranged, first, second, dens, ext, fh, fl, out1, out2, cols):
    odd = par[0] == 1
    left = ghosts[0, 0]
    ext[...] = extend(odd, arranged[0:6], first[...], second[...])
    for f in range(5):
        turned = ext[f].T
        for t in range(EXT):
            cols[f, t] = jnp.broadcast_to(turned[:, t : t + 1], (TILE, TILE))

    def tile(s, carry):
        own = [arranged[f, pl.ds(s, 1), :] for f in range(5)]
        x_i, y_i, z_i, _, h_i = [jnp.broadcast_to(v, (CHUNK, TILE)) for v in own]
        half = 0.5 / h_i
        total = jnp.zeros((CHUNK, TILE), F32)
        for n in range(NB):
            t = place_of(near[s, n], left)
            for c in range(TILE // CHUNK):
                rows = pl.ds(c * CHUNK, CHUNK)
                dx = cols[0, t, rows, :] - x_i
                dy = cols[1, t, rows, :] - y_i
                dz = cols[2, t, rows, :] - z_i
                r2 = dx * dx + dy * dy + dz * dz
                r = r2 * lax.rsqrt(jnp.maximum(r2, 1e-30))
                u = jnp.maximum(1.0 - r * half, 0.0)
                u2 = u * u
                total = total + (cols[3, t, rows, :] * (5.0 - 4.0 * u)) * (u2 * u2)
                reach = cols[4, t, rows, :] + h_i
                w = jnp.maximum(reach - r, 0.0)
                p2 = reach * reach
                p4 = p2 * p2
                force = (w * w * w) / (p4 * p4)
                high = force.astype(BF16)
                at = pl.ds(n * TILE + c * CHUNK, CHUNK)
                fh[s, at, :] = high
                fl[s, at, :] = (force - high.astype(F32)).astype(BF16)
        dens[pl.ds(s, 1), :] = jnp.sum(total, axis=0, keepdims=True)
        return carry

    lax.fori_loop(0, TD, tile, 0)
    h = arranged[4]
    density = KERNEL_NORM * dens[...] / (h * h * h)
    dens[...] = density
    send_parts(odd, density, out1, out2)


def weigh(near, left, fh, fl, vectors, staged, operand, result):
    count = len(vectors)
    used = 3 * count
    height = staged.shape[0] // EXT
    pieces = [split3(v) for v in vectors]
    for k in range(3):
        for q in range(count):
            staged[pl.ds(k * count + q, EXT, stride=height), :] = pieces[q][k]
    for q in range(used, height):
        staged[pl.ds(q, EXT, stride=height), :] = jnp.zeros((EXT, TILE), F32)
    for t in range(EXT):
        operand[t] = staged[t * height : (t + 1) * height, :].astype(BF16)
    for s in range(TD):
        row = jnp.concatenate([operand[place_of(near[s, n], left)] for n in range(NB)], axis=1)
        got = jnp.dot(row, fh[s], preferred_element_type=F32)
        got = got + jnp.dot(row, fl[s], preferred_element_type=F32)
        result[s * height : (s + 1) * height, :] = got
    sums = []
    for q in range(count):
        sums.append(
            sum(result[pl.ds(k * count + q, TD, stride=height), :] for k in (2, 1, 0))
        )
    return sums


def limiter_body(begin, *refs):
    if begin:
        (par, near, ghosts, arranged, ext, fh, fl, dens, d1, d2) = refs[:10]
        (diff, out1, out2, sums, fixed, dens_ext, staged, operand, result) = refs[10:]
        odd = par[0] == 1
        rho = extend(odd, dens[...], d1[...], d2[...])
        dens_ext[...] = rho
        e = ext[5]
    else:
        (par, near, ghosts, arranged, ext, fh, fl, dens_ext, fixed, energy, e1, e2) = refs[:12]
        (diff, out1, out2, sums, ext_energy, staged, operand, result) = refs[12:]
        odd = par[0] == 1
        rho = dens_ext[...]
        e = extend(odd, energy[...], e1[...], e2[...])
        ext_energy[...] = e
    left = ghosts[0, 0]
    v = (160.0 * KERNEL_NORM) * ext[3] / rho
    x = [ext[f] - 0.5 for f in range(3)]
    ve = v * e
    vectors = [ve] + [ve * x[f] for f in range(3)]
    if begin:
        vectors = vectors + [v] + [v * x[f] for f in range(3)]
    got = weigh(near, left, fh, fl, vectors, staged, operand, result)
    if begin:
        for q in range(4):
            fixed[q] = got[4 + q]
    base = [fixed[q] for q in range(4)]
    e_i = e[:TD]
    square = jnp.zeros((TD, TILE), F32)
    for f in range(3):
        x_i = x[f][:TD]
        grad = (got[1 + f] - x_i * got[0]) - e_i * (base[1 + f] - x_i * base[0])
        square = square + grad * grad
    thick = arranged[6] * rho[:TD]
    ratio = jnp.sqrt(square) / (thick * e_i)
    value = (2.0 + ratio) / ((6.0 + 3.0 * ratio + ratio * ratio) * thick)
    diff[...] = value
    sums[0] = base[0]
    sums[1] = got[0]
    send_parts(odd, value, out1, out2)


def jacobi_body(last, par, near, ghosts, arranged, ext, fh, fl, dens_ext, e_ext, sums, diff, d1, d2, *refs):
    if last:
        new, staged, operand, result = refs
    else:
        new, out1, out2, staged, operand, result = refs
    odd = par[0] == 1
    left = ghosts[0, 0]
    spread = extend(odd, diff[...], d1[...], d2[...])
    rho = dens_ext[...]
    vd = ((160.0 * KERNEL_NORM) * ext[3] / rho) * spread
    got = weigh(near, left, fh, fl, [vd, vd * e_ext[...]], staged, operand, result)
    own = spread[:TD]
    scale = TIME_STEP / rho[:TD]
    rate = scale * (own * sums[0] + got[0])
    inflow = scale * (own * sums[1] + got[1])
    value = (arranged[5] + TIME_STEP * arranged[7] + inflow) / (1.0 + rate)
    new[...] = value
    if not last:
        send_parts(odd, value, out1, out2)


def workspace(height):
    return [
        pltpu.VMEM((EXT * height, TILE), F32),
        pltpu.VMEM((EXT, height, TILE), BF16),
        pltpu.VMEM((TD * height, TILE), F32),
    ]


def swap(first, second):
    count = lax.axis_size("group") * lax.axis_size("member")
    odd = [(s, s + 1) for s in range(1, count - 1, 2)]
    even = [(s, s + 1) for s in range(0, count - 1, 2)]
    got = []
    for value, pairs in ((first, odd), (second, even)):
        got.append(lax.ppermute(value, AXES, pairs + [(b, a) for a, b in pairs]))
    return got


def local(particles, new_slot, neighbours, ghosts):
    groups = lax.axis_size("group")
    par = (lax.axis_index("member") % 2).astype(jnp.int32).reshape(1)
    (outgoing,) = call(
        pack_body,
        [((groups, ROWS, TILE), F32)],
        [pltpu.SMEM((groups,), jnp.int32)],
        "pack",
        new_slot,
        particles,
    )
    received = lax.all_to_all(outgoing, "group", split_axis=0, concat_axis=0, tiled=True)
    edge = ((GMAX, TILE), F32)
    own = ((TD, TILE), F32)
    wide = ((EXT, TILE), F32)
    arranged, s1, s2 = call(
        unpack_body,
        [((8, TD, TILE), F32), ((6, GMAX, TILE), F32), ((6, GMAX, TILE), F32)],
        [],
        "unpack",
        par,
        received.reshape(groups * ROWS, TILE),
    )
    table = (par, neighbours, ghosts)
    s1, s2 = swap(s1, s2)
    density, ext, fh, fl, r1, r2 = call(
        pairs_body,
        [
            own,
            ((6, EXT, TILE), F32),
            ((TD, NB * TILE, TILE), BF16),
            ((TD, NB * TILE, TILE), BF16),
            edge,
            edge,
        ],
        [pltpu.VMEM((5, EXT, TILE, TILE), F32)],
        "pairs",
        *table,
        arranged,
        s1,
        s2,
    )
    r1, r2 = swap(r1, r2)
    shared = (*table, arranged, ext, fh, fl)
    for step in range(SWEEPS):
        if step == 0:
            diff, d1, d2, sums, fixed, dens_ext = call(
                lambda *refs: limiter_body(True, *refs),
                [own, edge, edge, ((2, TD, TILE), F32), ((4, TD, TILE), F32), wide],
                workspace(32),
                "limiter_first",
                *shared,
                density,
                r1,
                r2,
            )
            e_ext = ext[5]
        else:
            diff, d1, d2, sums, e_ext = call(
                lambda *refs: limiter_body(False, *refs),
                [own, edge, edge, ((2, TD, TILE), F32), wide],
                workspace(16),
                "limiter",
                *shared,
                dens_ext,
                fixed,
                energy,
                e1,
                e2,
            )
        d1, d2 = swap(d1, d2)
        last = step == SWEEPS - 1
        results = call(
            lambda *refs: jacobi_body(last, *refs),
            [own] if last else [own, edge, edge],
            workspace(16),
            "jacobi",
            *shared,
            dens_ext,
            e_ext,
            sums,
            diff,
            d1,
            d2,
        )
        if last:
            energy = results[0]
        else:
            energy, e1, e2 = results
            e1, e2 = swap(e1, e2)
    return (energy.reshape(-1), density.reshape(-1))


def solution(mesh):
    in_specs = (
        P(None, ("group", "member")),
        P(("group", "member")),
        P(("group", "member"), None),
        P(("group", "member"), None),
    )
    out_specs = (P(("group", "member")), P(("group", "member")))
    return jax.shard_map(local, mesh=mesh, in_specs=in_specs, out_specs=out_specs, check_vma=False)
```

```python
import math

import jax
import jax.numpy as jnp
from jax import lax
from jax.experimental import pallas as pl
from jax.experimental.pallas import tpu as pltpu
from jax.sharding import PartitionSpec as P

TILE = 128
GMAX = 4
SWEEPS = 3
NB = 6
TD = 16
EXT = TD + 2 * GMAX
ROWS = 17
GROUPS = 32
DEPTH = 8
CHUNK = 32
KERNEL_NORM = 21.0 / (16.0 * math.pi)
TIME_STEP = 0.05
VMEM_LIMIT = 8 * 1024 * 1024
F32 = jnp.float32
BF16 = jnp.bfloat16
VMEM = pltpu.MemorySpace.VMEM
SMEM = pltpu.MemorySpace.SMEM
AXES = ("group", "member")


def call(body, outs, scratch, name, *args, alias={}):
    specs = [
        pl.BlockSpec(memory_space=SMEM if a.dtype == jnp.int32 else VMEM) for a in args
    ]
    return pl.pallas_call(
        body,
        out_shape=[jax.ShapeDtypeStruct(shape, dtype) for shape, dtype in outs],
        in_specs=specs,
        out_specs=[pl.BlockSpec(memory_space=VMEM) for _ in outs],
        scratch_shapes=scratch,
        name=name,
        input_output_aliases=alias,
        compiler_params=pltpu.CompilerParams(vmem_limit_bytes=VMEM_LIMIT),
    )(*args)


def owner(segment):
    group, member = divmod(segment, 8)
    if member in (5, 6):
        group = group // DEPTH * DEPTH + (group + 1) % DEPTH
    elif member == 7:
        group = (group + 1) % GROUPS
    return group * 8 + member


def pack_body(mem, slot_hbm, part_hbm, out, count, slot, part, sem):
    groups = out.shape[0] // ROWS
    slots = pltpu.make_async_copy(slot_hbm, slot, sem.at[0])
    parts = pltpu.make_async_copy(part_hbm, part, sem.at[1])
    slots.start()
    parts.start()
    out[...] = jnp.zeros(out.shape, F32)
    for g in range(groups):
        count[g] = 0
        out[g * ROWS + 16 : g * ROWS + 17, :] = jnp.full((1, TILE), -1.0, F32)
    lane = lax.broadcasted_iota(jnp.int32, (1, TILE), 1)
    m = mem[0]
    slots.wait()
    parts.wait()
    for t in range(TD):
        s = slot[t]
        g = s // (TD * 8)
        along = (g // DEPTH) * DEPTH + (g + 1) % DEPTH
        g = jnp.where(m < 5, g, jnp.where(m < 7, along, (g + 1) % groups))
        n = count[g]
        count[g] = n + 1
        base = g * ROWS
        for r in range(8):
            out[pl.ds(base + n * 8 + r, 1), :] = part[r : r + 1, t * TILE : (t + 1) * TILE]
        label = pl.ds(base + 16, 1)
        here = (lane // (TILE // 2)) == n
        out[label, :] = jnp.where(here, (s % TD).astype(F32), out[label, :])


def split3(x):
    hi = x.astype(BF16).astype(F32)
    rest = x - hi
    mid = rest.astype(BF16).astype(F32)
    return hi, mid, rest - mid


def send_parts(odd, values, first, second):
    n = values.shape[-2]
    tail = values[..., n - GMAX :, :]
    head = values[..., :GMAX, :]
    first[...] = jnp.where(odd, tail, head)
    second[...] = jnp.where(odd, head, tail)


def extend(odd, values, first, second):
    left = jnp.where(odd, second, first)
    right = jnp.where(odd, first, second)
    return jnp.concatenate([values, left, right], axis=-2)


def unpack_body(mem, got, arranged, first, second):
    groups = got.shape[0] // ROWS
    odd = mem[0] % 2 == 1
    lane = lax.broadcasted_iota(jnp.int32, (groups, TILE), 1).astype(F32)
    labels = got[pl.ds(16, groups, stride=ROWS), :]
    marks = [
        jnp.where(values == lane, 1.0, 0.0)
        for values in (labels, pltpu.roll(labels, TILE // 2, 1))
    ]
    marks.append(jnp.zeros((TILE - 2 * groups, TILE), F32))
    choose = jnp.concatenate(marks, axis=0).T[:TD, : 2 * groups].astype(BF16)
    for r in range(8):
        tiles = jnp.concatenate(
            [got[pl.ds(n * 8 + r, groups, stride=ROWS), :] for n in range(2)], axis=0
        )
        moved = sum(
            jnp.dot(choose, piece.astype(BF16), preferred_element_type=F32)
            for piece in split3(tiles)
        )
        arranged[r] = moved
    send_parts(odd, arranged[0:6], first, second)


def place_of(entry, left):
    j = entry - left
    return jnp.where(j < 0, j + TD + GMAX, jnp.where(j < TD, j, j + GMAX))


def spread_columns(cols, fields, tiles, first):
    for f in range(5):
        turned = fields[f].T
        for t in range(tiles):
            cols[f, first + t] = jnp.broadcast_to(turned[:, t : t + 1], (TILE, TILE))


def columns_body(arranged, cols):
    spread_columns(cols, [arranged[f] for f in range(5)], TD, 0)


def density_body(mem, near, arranged, first, second, held, dens, ext, dist, out1, out2, cols):
    odd = mem[0] % 2 == 1
    whole = extend(odd, arranged[0:6], first[...], second[...])
    ext[...] = whole
    spread_columns(cols, [whole[f, TD:] for f in range(5)], 2 * GMAX, TD)

    def tile(s, carry):
        own = [arranged[f, pl.ds(s, 1), :] for f in range(5)]
        x_i, y_i, z_i, _, h_i = [jnp.broadcast_to(v, (CHUNK, TILE)) for v in own]
        pace = 2.0 / h_i
        total = jnp.zeros((CHUNK, TILE), F32)
        for n in range(NB):
            t = near[s * NB + n]
            for c in range(TILE // CHUNK):
                rows = pl.ds(c * CHUNK, CHUNK)
                dx = cols[0, t, rows, :] - x_i
                dy = cols[1, t, rows, :] - y_i
                dz = cols[2, t, rows, :] - z_i
                r2 = dx * dx + dy * dy + dz * dz
                r = r2 * lax.rsqrt(jnp.maximum(r2, 1e-30))
                dist[s, pl.ds(n * TILE + c * CHUNK, CHUNK), :] = r
                u = jnp.maximum(4.0 - r * pace, 0.0)
                u2 = u * u
                total = total + (cols[3, t, rows, :] * (5.0 - u)) * (u2 * u2)
        dens[pl.ds(s, 1), :] = jnp.sum(total, axis=0, keepdims=True)
        return carry

    lax.fori_loop(0, TD, tile, 0)
    h = arranged[4]
    density = (KERNEL_NORM / 256.0) * dens[...] / (h * h * h)
    dens[...] = density
    send_parts(odd, density, out1, out2)


def forces_body(near, arranged, cols, dist, forces):
    def tile(s, carry):
        h_i = jnp.broadcast_to(arranged[4, pl.ds(s, 1), :], (CHUNK, TILE))
        for n in range(NB):
            t = near[s * NB + n]
            for c in range(TILE // CHUNK):
                at = pl.ds(n * TILE + c * CHUNK, CHUNK)
                reach = cols[4, t, pl.ds(c * CHUNK, CHUNK), :] + h_i
                w = jnp.maximum(reach - dist[s, at, :], 0.0)
                p2 = reach * reach
                q = w / (p2 * p2)
                force = q * q * w
                high = force.astype(BF16)
                forces[s, at, 0:TILE] = high
                forces[s, at, TILE : 2 * TILE] = (force - high.astype(F32)).astype(BF16)
        return carry

    lax.fori_loop(0, TD, tile, 0)


def weigh(near, forces, vectors, staged, operand, result):
    count = len(vectors)
    height = staged.shape[0] // EXT
    pieces = [split3(v) for v in vectors]
    for k in range(3):
        for q in range(count):
            staged[pl.ds(k * count + q, EXT, stride=height), :] = pieces[q][k]
    for t in range(EXT):
        operand[t] = staged[t * height : (t + 1) * height, :].astype(BF16)
    for s in range(TD):
        row = jnp.concatenate([operand[near[s * NB + n]] for n in range(NB)], axis=1)
        got = jnp.dot(row, forces[s], preferred_element_type=F32)
        result[s * height : (s + 1) * height, :] = got[:, TILE:] + got[:, :TILE]
    sums = []
    for q in range(count):
        sums.append(
            sum(result[pl.ds(k * count + q, TD, stride=height), :] for k in (2, 1, 0))
        )
    return sums


def limiter_body(begin, *refs):
    if begin:
        (mem, near, arranged, ext, forces, dens, d1, d2) = refs[:8]
        (diff, out1, out2, sums, fixed, dens_ext, staged, operand, result) = refs[8:]
        odd = mem[0] % 2 == 1
        rho = extend(odd, dens[...], d1[...], d2[...])
        dens_ext[...] = rho
        e = ext[5]
    else:
        (mem, near, arranged, ext, forces, dens_ext, fixed, energy, e1, e2) = refs[:10]
        (diff, out1, out2, sums, ext_energy, staged, operand, result) = refs[10:]
        odd = mem[0] % 2 == 1
        rho = dens_ext[...]
        e = extend(odd, energy[...], e1[...], e2[...])
        ext_energy[...] = e
    v = (160.0 * KERNEL_NORM) * ext[3] / rho
    x = [ext[f] - 0.5 for f in range(3)]
    ve = v * e
    vectors = [ve] + [ve * x[f] for f in range(3)]
    if begin:
        vectors = vectors + [v] + [v * x[f] for f in range(3)]
    got = weigh(near, forces, vectors, staged, operand, result)
    if begin:
        for q in range(4):
            fixed[q] = got[4 + q]
    base = [fixed[q] for q in range(4)]
    e_i = e[:TD]
    square = jnp.zeros((TD, TILE), F32)
    for f in range(3):
        x_i = x[f][:TD]
        grad = (got[1 + f] - x_i * got[0]) - e_i * (base[1 + f] - x_i * base[0])
        square = square + grad * grad
    thick = arranged[6] * rho[:TD]
    ratio = jnp.sqrt(square) / (thick * e_i)
    value = (2.0 + ratio) / ((6.0 + 3.0 * ratio + ratio * ratio) * thick)
    diff[...] = value
    sums[0] = base[0]
    sums[1] = got[0]
    send_parts(odd, value, out1, out2)


def jacobi_body(last, mem, near, arranged, ext, forces, dens_ext, e_ext, sums, diff, d1, d2, *refs):
    if last:
        dens, new, staged, operand, result = refs
    else:
        new, out1, out2, staged, operand, result = refs
    odd = mem[0] % 2 == 1
    spread = extend(odd, diff[...], d1[...], d2[...])
    rho = dens_ext[...]
    vd = ((160.0 * KERNEL_NORM) * ext[3] / rho) * spread
    got = weigh(near, forces, [vd, vd * e_ext[...]], staged, operand, result)
    own = spread[:TD]
    scale = TIME_STEP / rho[:TD]
    rate = scale * (own * sums[0] + got[0])
    inflow = scale * (own * sums[1] + got[1])
    value = (arranged[5] + TIME_STEP * arranged[7] + inflow) / (1.0 + rate)
    new[:TD] = value
    if last:
        new[TD:] = dens[...]
    else:
        send_parts(odd, value, out1, out2)


def workspace(height):
    return [
        pltpu.VMEM((EXT * height, TILE), F32),
        pltpu.VMEM((EXT, height, TILE), BF16),
        pltpu.VMEM((TD * height, TILE), F32),
    ]


def swap(first, second):
    odd = [(owner(s), owner(s + 1)) for s in range(1, GROUPS * 8 - 1, 2)]
    even = [(owner(s), owner(s + 1)) for s in range(0, GROUPS * 8 - 1, 2)]
    got = []
    for value, pairs in ((first, odd), (second, even)):
        got.append(lax.ppermute(value, AXES, pairs + [(b, a) for a, b in pairs]))
    return got


def local(particles, new_slot, neighbours, ghosts):
    mem = lax.axis_index("member").astype(jnp.int32).reshape(1)
    outgoing = pl.pallas_call(
        pack_body,
        out_shape=jax.ShapeDtypeStruct((GROUPS * ROWS, TILE), F32),
        in_specs=[
            pl.BlockSpec(memory_space=SMEM),
            pl.BlockSpec(memory_space=pltpu.MemorySpace.HBM),
            pl.BlockSpec(memory_space=pltpu.MemorySpace.HBM),
        ],
        out_specs=pl.BlockSpec(memory_space=VMEM),
        scratch_shapes=[
            pltpu.SMEM((GROUPS,), jnp.int32),
            pltpu.SMEM((TD,), jnp.int32),
            pltpu.VMEM((8, TD * TILE), F32),
            pltpu.SemaphoreType.DMA((2,)),
        ],
        name="pack",
        compiler_params=pltpu.CompilerParams(vmem_limit_bytes=VMEM_LIMIT),
    )(mem, new_slot, particles)
    received = lax.all_to_all(
        outgoing.reshape(GROUPS * ROWS, 1, TILE), "group", split_axis=0, concat_axis=0, tiled=True
    )
    near = place_of(neighbours, ghosts[0, 0]).reshape(TD * NB)
    near = lax.ppermute(near, AXES, [(s, owner(s)) for s in range(GROUPS * 8)])
    edge = ((GMAX, TILE), F32)
    own = ((TD, TILE), F32)
    wide = ((EXT, TILE), F32)
    arranged, s1, s2 = call(
        unpack_body,
        [((8, TD, TILE), F32), ((6, GMAX, TILE), F32), ((6, GMAX, TILE), F32)],
        [],
        "unpack",
        mem,
        received.reshape(GROUPS * ROWS, TILE),
    )
    table = (mem, near)
    s1, s2 = swap(s1, s2)
    (cols,) = call(columns_body, [((5, EXT, TILE, TILE), F32)], [], "columns", arranged)
    density, ext, dist, r1, r2, cols = call(
        density_body,
        [
            own,
            ((6, EXT, TILE), F32),
            ((TD, NB * TILE, TILE), F32),
            edge,
            edge,
            ((5, EXT, TILE, TILE), F32),
        ],
        [],
        "density",
        *table,
        arranged,
        s1,
        s2,
        cols,
        alias={5: 5},
    )
    r1, r2 = swap(r1, r2)
    (forces,) = call(
        forces_body,
        [((TD, NB * TILE, 2 * TILE), BF16)],
        [],
        "forces",
        near,
        arranged,
        cols,
        dist,
    )
    shared = (*table, arranged, ext, forces)
    for step in range(SWEEPS):
        if step == 0:
            diff, d1, d2, sums, fixed, dens_ext = call(
                lambda *refs: limiter_body(True, *refs),
                [own, edge, edge, ((2, TD, TILE), F32), ((4, TD, TILE), F32), wide],
                workspace(24),
                "limiter_first",
                *shared,
                density,
                r1,
                r2,
            )
            e_ext = ext[5]
        else:
            diff, d1, d2, sums, e_ext = call(
                lambda *refs: limiter_body(False, *refs),
                [own, edge, edge, ((2, TD, TILE), F32), wide],
                workspace(16),
                "limiter",
                *shared,
                dens_ext,
                fixed,
                energy,
                e1,
                e2,
            )
        d1, d2 = swap(d1, d2)
        last = step == SWEEPS - 1
        results = call(
            lambda *refs: jacobi_body(last, *refs),
            [((2 * TD, TILE), F32)] if last else [own, edge, edge],
            workspace(8),
            "jacobi",
            *shared,
            dens_ext,
            e_ext,
            sums,
            diff,
            d1,
            d2,
            *((density,) if last else ()),
        )
        if last:
            done = results[0]
        else:
            energy, e1, e2 = results
            e1, e2 = swap(e1, e2)
    done = lax.ppermute(done, AXES, [(owner(s), s) for s in range(GROUPS * 8)])
    return (done[:TD].reshape(-1), done[TD:].reshape(-1))


def solution(mesh):
    in_specs = (
        P(None, ("group", "member")),
        P(("group", "member")),
        P(("group", "member"), None),
        P(("group", "member"), None),
    )
    out_specs = (P(("group", "member")), P(("group", "member")))
    return jax.shard_map(local, mesh=mesh, in_specs=in_specs, out_specs=out_specs, check_vma=False)
```

```python
import math

import jax
import jax.numpy as jnp
from jax import lax
from jax.experimental import pallas as pl
from jax.experimental.pallas import tpu as pltpu
from jax.sharding import PartitionSpec as P

TILE = 128
GMAX = 4
SWEEPS = 3
NB = 6
TD = 16
EXT = TD + 2 * GMAX
ROWS = 17
GROUPS = 32
DEPTH = 8
LIST = 32
CHUNK = 32
KERNEL_NORM = 21.0 / (16.0 * math.pi)
TIME_STEP = 0.05
VMEM_LIMIT = 8 * 1024 * 1024
F32 = jnp.float32
BF16 = jnp.bfloat16
VMEM = pltpu.MemorySpace.VMEM
SMEM = pltpu.MemorySpace.SMEM
AXES = ("group", "member")


def call(body, outs, scratch, name, *args, alias={}):
    specs = [
        pl.BlockSpec(memory_space=SMEM if a.dtype == jnp.int32 else VMEM) for a in args
    ]
    return pl.pallas_call(
        body,
        out_shape=[jax.ShapeDtypeStruct(shape, dtype) for shape, dtype in outs],
        in_specs=specs,
        out_specs=[pl.BlockSpec(memory_space=VMEM) for _ in outs],
        scratch_shapes=scratch,
        name=name,
        input_output_aliases=alias,
        compiler_params=pltpu.CompilerParams(vmem_limit_bytes=VMEM_LIMIT),
    )(*args)


def owner(segment):
    group, member = divmod(segment, 8)
    if member in (5, 6):
        group = group // DEPTH * DEPTH + (group + 1) % DEPTH
    elif member == 7:
        group = (group + 1) % GROUPS
    return group * 8 + member


def moved_group(group, member):
    along = (group // DEPTH) * DEPTH + (group + 1) % DEPTH
    return jnp.where(member < 5, group, jnp.where(member < 7, along, (group + 1) % GROUPS))


def home_group(group, member):
    along = (group // DEPTH) * DEPTH + (group + DEPTH - 1) % DEPTH
    far = (group + GROUPS - 1) % GROUPS
    return jnp.where(member < 5, group, jnp.where(member < 7, along, far))


def pack_body(grp, mem, ghosts_hbm, slot_hbm, near_hbm, part_hbm, out, count, ghosts, slot, near, part, sem):
    copies = [
        pltpu.make_async_copy(source, target, sem.at[k])
        for k, (source, target) in enumerate(
            [(ghosts_hbm, ghosts), (slot_hbm, slot), (near_hbm, near), (part_hbm, part)]
        )
    ]
    for copy in copies:
        copy.start()
    out[...] = jnp.zeros(out.shape, F32)
    for g in range(GROUPS):
        count[g] = 0
        out[g * ROWS + 16 : g * ROWS + 17, :] = jnp.full((1, TILE), -1.0, F32)
    lane = lax.broadcasted_iota(jnp.int32, (1, TILE), 1)
    m = mem[0]
    for copy in copies:
        copy.wait()
    place = place_of(near[...], ghosts[0, 0]).astype(F32)
    row = jnp.full((1, TILE), -1.0, F32)
    for n in range(NB):
        first = LIST + n * TD
        piece = jnp.concatenate([place[n : n + 1], jnp.zeros((1, TILE - TD), F32)], axis=1)
        row = jnp.where((lane >= first) & (lane < first + TD), pltpu.roll(piece, first, 1), row)
    out[pl.ds(moved_group(grp[0], m) * ROWS + 16, 1), :] = row
    for t in range(TD):
        s = slot[t]
        g = moved_group(s // (TD * 8), m)
        n = count[g]
        count[g] = n + 1
        base = g * ROWS
        for r in range(8):
            out[pl.ds(base + n * 8 + r, 1), :] = part[r : r + 1, t * TILE : (t + 1) * TILE]
        label = pl.ds(base + 16, 1)
        here = (lane >= n * TD) & (lane < n * TD + TD)
        out[label, :] = jnp.where(here, (s % TD).astype(F32), out[label, :])


def split3(x):
    hi = x.astype(BF16).astype(F32)
    rest = x - hi
    mid = rest.astype(BF16).astype(F32)
    return hi, mid, rest - mid


def send_parts(odd, values, first, second):
    n = values.shape[-2]
    tail = values[..., n - GMAX :, :]
    head = values[..., :GMAX, :]
    first[...] = jnp.where(odd, head, tail)
    second[...] = jnp.where(odd, tail, head)


def extend(odd, values, first, second):
    left = jnp.where(odd, first, second)
    right = jnp.where(odd, second, first)
    return jnp.concatenate([values, left, right], axis=-2)


def unpack_body(grp, mem, got, arranged, first, second, table):
    groups = got.shape[0] // ROWS
    odd = mem[0] % 2 == 1
    lane = lax.broadcasted_iota(jnp.int32, (groups, TILE), 1).astype(F32)
    labels = got[pl.ds(16, groups, stride=ROWS), :]
    marks = [
        jnp.where(values == lane, 1.0, 0.0)
        for values in (labels, pltpu.roll(labels, TILE - TD, 1))
    ]
    marks.append(jnp.zeros((TILE - 2 * groups, TILE), F32))
    choose = jnp.concatenate(marks, axis=0).T[:TD, : 2 * groups].astype(BF16)
    for r in range(8):
        tiles = jnp.concatenate(
            [got[pl.ds(n * 8 + r, groups, stride=ROWS), :] for n in range(2)], axis=0
        )
        moved = sum(
            jnp.dot(choose, piece.astype(BF16), preferred_element_type=F32)
            for piece in split3(tiles)
        )
        arranged[r] = moved
    mine = pl.ds(home_group(grp[0], mem[0]) * ROWS + 16, 1)
    table[...] = got[mine, :].astype(jnp.int32)
    send_parts(odd, arranged[0:6], first, second)


def place_of(entry, left):
    j = entry - left
    return jnp.where(j < 0, j + TD + GMAX, jnp.where(j < TD, j, j + GMAX))


def spread_columns(cols, fields, tiles, first):
    for f in range(5):
        turned = fields[f].T
        for t in range(tiles):
            cols[f, first + t] = jnp.broadcast_to(turned[:, t : t + 1], (TILE, TILE))


def columns_body(arranged, cols):
    spread_columns(cols, [arranged[f] for f in range(5)], TD, 0)


def density_body(mem, near, arranged, first, second, held, dens, ext, dist, out1, out2, cols):
    odd = mem[0] % 2 == 1
    whole = extend(odd, arranged[0:6], first[...], second[...])
    ext[...] = whole
    spread_columns(cols, [whole[f, TD:] for f in range(5)], 2 * GMAX, TD)

    def tile(s, carry):
        own = [arranged[f, pl.ds(s, 1), :] for f in range(5)]
        x_i, y_i, z_i, _, h_i = [jnp.broadcast_to(v, (CHUNK, TILE)) for v in own]
        pace = 2.0 / h_i
        total = jnp.zeros((CHUNK, TILE), F32)
        for n in range(NB):
            t = near[0, LIST + n * TD + s]
            for c in range(TILE // CHUNK):
                rows = pl.ds(c * CHUNK, CHUNK)
                dx = cols[0, t, rows, :] - x_i
                dy = cols[1, t, rows, :] - y_i
                dz = cols[2, t, rows, :] - z_i
                r2 = dx * dx + dy * dy + dz * dz
                r = r2 * lax.rsqrt(jnp.maximum(r2, 1e-30))
                dist[s, pl.ds(n * TILE + c * CHUNK, CHUNK), :] = r
                u = jnp.maximum(4.0 - r * pace, 0.0)
                u2 = u * u
                total = total + (cols[3, t, rows, :] * (5.0 - u)) * (u2 * u2)
        dens[pl.ds(s, 1), :] = jnp.sum(total, axis=0, keepdims=True)
        return carry

    lax.fori_loop(0, TD, tile, 0)
    h = arranged[4]
    density = (KERNEL_NORM / 256.0) * dens[...] / (h * h * h)
    dens[...] = density
    send_parts(odd, density, out1, out2)


def forces_body(near, arranged, cols, dist, forces):
    def tile(s, carry):
        h_i = jnp.broadcast_to(arranged[4, pl.ds(s, 1), :], (CHUNK, TILE))
        for n in range(NB):
            t = near[0, LIST + n * TD + s]
            for c in range(TILE // CHUNK):
                at = pl.ds(n * TILE + c * CHUNK, CHUNK)
                reach = cols[4, t, pl.ds(c * CHUNK, CHUNK), :] + h_i
                w = jnp.maximum(reach - dist[s, at, :], 0.0)
                p2 = reach * reach
                q = w / (p2 * p2)
                force = q * q * w
                high = force.astype(BF16)
                forces[s, at, 0:TILE] = high
                forces[s, at, TILE : 2 * TILE] = (force - high.astype(F32)).astype(BF16)
        return carry

    lax.fori_loop(0, TD, tile, 0)


def weigh(near, forces, vectors, staged, operand, result):
    count = len(vectors)
    height = staged.shape[0] // EXT
    pieces = [split3(v) for v in vectors]
    for k in range(3):
        for q in range(count):
            staged[pl.ds(k * count + q, EXT, stride=height), :] = pieces[q][k]
    for t in range(EXT):
        operand[t] = staged[t * height : (t + 1) * height, :].astype(BF16)
    for s in range(TD):
        row = jnp.concatenate([operand[near[0, LIST + n * TD + s]] for n in range(NB)], axis=1)
        got = jnp.dot(row, forces[s], preferred_element_type=F32)
        result[s * height : (s + 1) * height, :] = got[:, TILE:] + got[:, :TILE]
    sums = []
    for q in range(count):
        sums.append(
            sum(result[pl.ds(k * count + q, TD, stride=height), :] for k in (2, 1, 0))
        )
    return sums


def limiter_body(begin, *refs):
    if begin:
        (mem, near, arranged, ext, forces, dens, d1, d2) = refs[:8]
        (diff, out1, out2, sums, fixed, dens_ext, staged, operand, result) = refs[8:]
        odd = mem[0] % 2 == 1
        rho = extend(odd, dens[...], d1[...], d2[...])
        dens_ext[...] = rho
        e = ext[5]
    else:
        (mem, near, arranged, ext, forces, dens_ext, fixed, energy, e1, e2) = refs[:10]
        (diff, out1, out2, sums, ext_energy, staged, operand, result) = refs[10:]
        odd = mem[0] % 2 == 1
        rho = dens_ext[...]
        e = extend(odd, energy[...], e1[...], e2[...])
        ext_energy[...] = e
    v = (160.0 * KERNEL_NORM) * ext[3] / rho
    x = [ext[f] - 0.5 for f in range(3)]
    ve = v * e
    vectors = [ve] + [ve * x[f] for f in range(3)]
    if begin:
        vectors = vectors + [v] + [v * x[f] for f in range(3)]
    got = weigh(near, forces, vectors, staged, operand, result)
    if begin:
        for q in range(4):
            fixed[q] = got[4 + q]
    base = [fixed[q] for q in range(4)]
    e_i = e[:TD]
    square = jnp.zeros((TD, TILE), F32)
    for f in range(3):
        x_i = x[f][:TD]
        grad = (got[1 + f] - x_i * got[0]) - e_i * (base[1 + f] - x_i * base[0])
        square = square + grad * grad
    thick = arranged[6] * rho[:TD]
    ratio = jnp.sqrt(square) / (thick * e_i)
    value = (2.0 + ratio) / ((6.0 + 3.0 * ratio + ratio * ratio) * thick)
    diff[...] = value
    sums[0] = base[0]
    sums[1] = got[0]
    send_parts(odd, value, out1, out2)


def jacobi_body(last, mem, near, arranged, ext, forces, dens_ext, e_ext, sums, diff, d1, d2, *refs):
    if last:
        dens, new, staged, operand, result = refs
    else:
        new, out1, out2, staged, operand, result = refs
    odd = mem[0] % 2 == 1
    spread = extend(odd, diff[...], d1[...], d2[...])
    rho = dens_ext[...]
    vd = ((160.0 * KERNEL_NORM) * ext[3] / rho) * spread
    got = weigh(near, forces, [vd, vd * e_ext[...]], staged, operand, result)
    own = spread[:TD]
    scale = TIME_STEP / rho[:TD]
    rate = scale * (own * sums[0] + got[0])
    inflow = scale * (own * sums[1] + got[1])
    value = (arranged[5] + TIME_STEP * arranged[7] + inflow) / (1.0 + rate)
    new[:TD] = value
    if last:
        new[TD:] = dens[...]
    else:
        send_parts(odd, value, out1, out2)


def workspace(height):
    return [
        pltpu.VMEM((EXT * height, TILE), F32),
        pltpu.VMEM((EXT, height, TILE), BF16),
        pltpu.VMEM((TD * height, TILE), F32),
    ]


def swap(first, second):
    odd = [(owner(s), owner(s + 1)) for s in range(1, GROUPS * 8 - 1, 2)]
    even = [(owner(s), owner(s + 1)) for s in range(0, GROUPS * 8 - 1, 2)]
    got = []
    for value, pairs in ((first, even), (second, odd)):
        got.append(lax.ppermute(value, AXES, pairs + [(b, a) for a, b in pairs]))
    return got


def local(particles, new_slot, neighbours, ghosts):
    grp, mem = [lax.axis_index(axis).astype(jnp.int32).reshape(1) for axis in AXES]
    hbm = pl.BlockSpec(memory_space=pltpu.MemorySpace.HBM)
    outgoing = pl.pallas_call(
        pack_body,
        out_shape=jax.ShapeDtypeStruct((GROUPS * ROWS, TILE), F32),
        in_specs=[
            pl.BlockSpec(memory_space=SMEM),
            pl.BlockSpec(memory_space=SMEM),
            hbm,
            hbm,
            hbm,
            hbm,
        ],
        out_specs=pl.BlockSpec(memory_space=VMEM),
        scratch_shapes=[
            pltpu.SMEM((GROUPS,), jnp.int32),
            pltpu.SMEM((1, 2), jnp.int32),
            pltpu.SMEM((TD,), jnp.int32),
            pltpu.VMEM((NB, TD), jnp.int32),
            pltpu.VMEM((8, TD * TILE), F32),
            pltpu.SemaphoreType.DMA((4,)),
        ],
        name="pack",
        compiler_params=pltpu.CompilerParams(vmem_limit_bytes=VMEM_LIMIT),
    )(
        grp,
        mem,
        *(
            pltpu.with_memory_space_constraint(a, pltpu.MemorySpace.HBM)
            for a in (ghosts, new_slot, neighbours.T, particles)
        ),
    )
    received = lax.all_to_all(
        outgoing.reshape(GROUPS * ROWS, 1, TILE), "group", split_axis=0, concat_axis=0, tiled=True
    )
    edge = ((GMAX, TILE), F32)
    own = ((TD, TILE), F32)
    wide = ((EXT, TILE), F32)
    arranged, s1, s2, near = call(
        unpack_body,
        [
            ((8, TD, TILE), F32),
            ((6, GMAX, TILE), F32),
            ((6, GMAX, TILE), F32),
            ((1, TILE), jnp.int32),
        ],
        [],
        "unpack",
        grp,
        mem,
        received.reshape(GROUPS * ROWS, TILE),
    )
    table = (mem, near)
    s1, s2 = swap(s1, s2)
    (cols,) = call(columns_body, [((5, EXT, TILE, TILE), F32)], [], "columns", arranged)
    density, ext, dist, r1, r2, cols = call(
        density_body,
        [
            own,
            ((6, EXT, TILE), F32),
            ((TD, NB * TILE, TILE), F32),
            edge,
            edge,
            ((5, EXT, TILE, TILE), F32),
        ],
        [],
        "density",
        *table,
        arranged,
        s1,
        s2,
        cols,
        alias={5: 5},
    )
    r1, r2 = swap(r1, r2)
    (forces,) = call(
        forces_body,
        [((TD, NB * TILE, 2 * TILE), BF16)],
        [],
        "forces",
        near,
        arranged,
        cols,
        dist,
    )
    shared = (*table, arranged, ext, forces)
    for step in range(SWEEPS):
        if step == 0:
            diff, d1, d2, sums, fixed, dens_ext = call(
                lambda *refs: limiter_body(True, *refs),
                [own, edge, edge, ((2, TD, TILE), F32), ((4, TD, TILE), F32), wide],
                workspace(24),
                "limiter_first",
                *shared,
                density,
                r1,
                r2,
            )
            e_ext = ext[5]
        else:
            diff, d1, d2, sums, e_ext = call(
                lambda *refs: limiter_body(False, *refs),
                [own, edge, edge, ((2, TD, TILE), F32), wide],
                workspace(16),
                "limiter",
                *shared,
                dens_ext,
                fixed,
                energy,
                e1,
                e2,
            )
        d1, d2 = swap(d1, d2)
        last = step == SWEEPS - 1
        results = call(
            lambda *refs: jacobi_body(last, *refs),
            [((2 * TD, TILE), F32)] if last else [own, edge, edge],
            workspace(8),
            "jacobi",
            *shared,
            dens_ext,
            e_ext,
            sums,
            diff,
            d1,
            d2,
            *((density,) if last else ()),
        )
        if last:
            done = results[0]
        else:
            energy, e1, e2 = results
            e1, e2 = swap(e1, e2)
    done = lax.ppermute(done, AXES, [(owner(s), s) for s in range(GROUPS * 8)])
    return (done[:TD].reshape(-1), done[TD:].reshape(-1))


def solution(mesh):
    in_specs = (
        P(None, ("group", "member")),
        P(("group", "member")),
        P(("group", "member"), None),
        P(("group", "member"), None),
    )
    out_specs = (P(("group", "member")), P(("group", "member")))
    return jax.shard_map(local, mesh=mesh, in_specs=in_specs, out_specs=out_specs, check_vma=False)
```

```python
import math

import jax
import jax.numpy as jnp
from jax import lax
from jax.experimental import pallas as pl
from jax.experimental.pallas import tpu as pltpu
from jax.sharding import PartitionSpec as P

TILE = 128
GMAX = 4
SWEEPS = 3
NB = 6
TD = 16
EXT = TD + 2 * GMAX
ROWS = 17
GROUPS = 32
DEPTH = 8
LIST = 32
HALF = TD // 2
CHUNK = 32
KERNEL_NORM = 21.0 / (16.0 * math.pi)
TIME_STEP = 0.05
VMEM_LIMIT = 8 * 1024 * 1024
F32 = jnp.float32
BF16 = jnp.bfloat16
VMEM = pltpu.MemorySpace.VMEM
SMEM = pltpu.MemorySpace.SMEM
AXES = ("group", "member")


def call(body, outs, scratch, name, *args, alias={}):
    specs = [
        pl.BlockSpec(memory_space=SMEM if a.shape == (1,) else VMEM) for a in args
    ]
    return pl.pallas_call(
        body,
        out_shape=[jax.ShapeDtypeStruct(shape, dtype) for shape, dtype in outs],
        in_specs=specs,
        out_specs=[pl.BlockSpec(memory_space=VMEM) for _ in outs],
        scratch_shapes=scratch,
        name=name,
        input_output_aliases=alias,
        compiler_params=pltpu.CompilerParams(vmem_limit_bytes=VMEM_LIMIT),
    )(*args)


def owner(segment):
    group, member = divmod(segment, 8)
    if member in (5, 6):
        group = group // DEPTH * DEPTH + (group + 1) % DEPTH
    elif member == 7:
        group = (group + 1) % GROUPS
    return group * 8 + member


def moved_group(group, member):
    along = (group // DEPTH) * DEPTH + (group + 1) % DEPTH
    return jnp.where(member < 5, group, jnp.where(member < 7, along, (group + 1) % GROUPS))


def home_group(group, member):
    along = (group // DEPTH) * DEPTH + (group + DEPTH - 1) % DEPTH
    far = (group + GROUPS - 1) % GROUPS
    return jnp.where(member < 5, group, jnp.where(member < 7, along, far))


def pack_body(grp, mem, ghosts_hbm, slot_hbm, near_hbm, part_hbm, out, count, ghosts, slot, near, part, sem):
    copies = [
        pltpu.make_async_copy(source, target, sem.at[k])
        for k, (source, target) in enumerate(
            [(ghosts_hbm, ghosts), (slot_hbm, slot), (near_hbm, near), (part_hbm, part)]
        )
    ]
    for copy in copies:
        copy.start()
    out[...] = jnp.zeros(out.shape, F32)
    for g in range(GROUPS):
        count[g] = 0
        out[g * ROWS + 16 : g * ROWS + 17, :] = jnp.full((1, TILE), -1.0, F32)
    lane = lax.broadcasted_iota(jnp.int32, (1, TILE), 1)
    m = mem[0]
    for copy in copies:
        copy.wait()
    place = place_of(near[...], ghosts[0, 0]).astype(F32)
    place = jnp.concatenate(
        [place[:, GMAX : GMAX + HALF], place[:, :GMAX], place[:, GMAX + HALF :]], axis=1
    )
    row = jnp.full((1, TILE), -1.0, F32)
    for n in range(NB):
        first = LIST + n * TD
        piece = jnp.concatenate([place[n : n + 1], jnp.zeros((1, TILE - TD), F32)], axis=1)
        row = jnp.where((lane >= first) & (lane < first + TD), pltpu.roll(piece, first, 1), row)
    out[pl.ds(moved_group(grp[0], m) * ROWS + 16, 1), :] = row
    for t in range(TD):
        s = slot[t]
        g = moved_group(s // (TD * 8), m)
        n = count[g]
        count[g] = n + 1
        base = g * ROWS
        for r in range(8):
            out[pl.ds(base + n * 8 + r, 1), :] = part[r : r + 1, t * TILE : (t + 1) * TILE]
        label = pl.ds(base + 16, 1)
        here = (lane >= n * TD) & (lane < n * TD + TD)
        out[label, :] = jnp.where(here, rank(s % TD).astype(F32), out[label, :])


def split3(x):
    hi = x.astype(BF16).astype(F32)
    rest = x - hi
    mid = rest.astype(BF16).astype(F32)
    return hi, mid, rest - mid


def send_parts(odd, values, first, second):
    n = values.shape[-2]
    tail = values[..., n - GMAX :, :]
    head = values[..., n - HALF : n - GMAX, :]
    first[...] = jnp.where(odd, head, tail)
    second[...] = jnp.where(odd, tail, head)


def extend(odd, values, first, second):
    left = jnp.where(odd, first, second)
    right = jnp.where(odd, second, first)
    return jnp.concatenate([values, left, right], axis=-2)


def unpack_body(grp, mem, got, arranged, first, second, table):
    groups = got.shape[0] // ROWS
    odd = mem[0] % 2 == 1
    lane = lax.broadcasted_iota(jnp.int32, (groups, TILE), 1).astype(F32)
    labels = got[pl.ds(16, groups, stride=ROWS), :]
    marks = [
        jnp.where(values == lane, 1.0, 0.0)
        for values in (labels, pltpu.roll(labels, TILE - TD, 1))
    ]
    marks.append(jnp.zeros((TILE - 2 * groups, TILE), F32))
    choose = jnp.concatenate(marks, axis=0).T[:TD, : 2 * groups].astype(BF16)
    for r in range(8):
        tiles = jnp.concatenate(
            [got[pl.ds(n * 8 + r, groups, stride=ROWS), :] for n in range(2)], axis=0
        )
        moved = sum(
            jnp.dot(choose, piece.astype(BF16), preferred_element_type=F32)
            for piece in split3(tiles)
        )
        arranged[r] = moved
    mine = pl.ds(home_group(grp[0], mem[0]) * ROWS + 16, 1)
    table[...] = got[mine, :].astype(jnp.int32)
    send_parts(odd, arranged[0:6], first, second)


def place_of(entry, left):
    j = entry - left
    return jnp.where(j < 0, j + TD + GMAX, jnp.where(j < TD, rank(j), j + GMAX))


def rank(tile):
    return jnp.where(tile < GMAX, tile + HALF, jnp.where(tile < GMAX + HALF, tile - GMAX, tile))


LISTED = [pltpu.SMEM((1, TILE), jnp.int32), pltpu.SemaphoreType.DMA]


def spread_columns(cols, fields, tiles, first):
    for f in range(5):
        turned = fields[f].T
        for t in range(tiles):
            cols[f, first + t] = jnp.broadcast_to(turned[:, t : t + 1], (TILE, TILE))


def columns_body(arranged, cols):
    spread_columns(cols, [arranged[f] for f in range(5)], TD, 0)


def density_body(
    mem, table, arranged, first, second, held, dens, ext, dist, out1, out2, cols, near, sem
):
    listed = pltpu.make_async_copy(table, near, sem)
    listed.start()
    odd = mem[0] % 2 == 1
    whole = extend(odd, arranged[0:6], first[...], second[...])
    ext[...] = whole
    spread_columns(cols, [whole[f, TD:] for f in range(5)], 2 * GMAX, TD)
    listed.wait()

    def tile(s, carry):
        own = [arranged[f, pl.ds(s, 1), :] for f in range(5)]
        x_i, y_i, z_i, _, h_i = [jnp.broadcast_to(v, (CHUNK, TILE)) for v in own]
        pace = 2.0 / h_i
        total = jnp.zeros((CHUNK, TILE), F32)
        for n in range(NB):
            t = near[0, LIST + n * TD + s]
            for c in range(TILE // CHUNK):
                rows = pl.ds(c * CHUNK, CHUNK)
                dx = cols[0, t, rows, :] - x_i
                dy = cols[1, t, rows, :] - y_i
                dz = cols[2, t, rows, :] - z_i
                r2 = dx * dx + dy * dy + dz * dz
                r = r2 * lax.rsqrt(jnp.maximum(r2, 1e-30))
                dist[s, pl.ds(n * TILE + c * CHUNK, CHUNK), :] = r
                u = jnp.maximum(4.0 - r * pace, 0.0)
                u2 = u * u
                total = total + (cols[3, t, rows, :] * (5.0 - u)) * (u2 * u2)
        dens[pl.ds(s, 1), :] = jnp.sum(total, axis=0, keepdims=True)
        return carry

    lax.fori_loop(0, TD, tile, 0)
    h = arranged[4]
    density = (KERNEL_NORM / 256.0) * dens[...] / (h * h * h)
    dens[...] = density
    send_parts(odd, density, out1, out2)


def forces_body(table, arranged, cols, dist, forces, near, sem):
    listed = pltpu.make_async_copy(table, near, sem)
    listed.start()
    listed.wait()

    def tile(s, carry):
        h_i = jnp.broadcast_to(arranged[4, pl.ds(s, 1), :], (CHUNK, TILE))
        for n in range(NB):
            t = near[0, LIST + n * TD + s]
            for c in range(TILE // CHUNK):
                at = pl.ds(n * TILE + c * CHUNK, CHUNK)
                reach = cols[4, t, pl.ds(c * CHUNK, CHUNK), :] + h_i
                w = jnp.maximum(reach - dist[s, at, :], 0.0)
                p2 = reach * reach
                q = w / (p2 * p2)
                force = q * q * w
                high = force.astype(BF16)
                forces[s, at, 0:TILE] = high
                forces[s, at, TILE : 2 * TILE] = (force - high.astype(F32)).astype(BF16)
        return carry

    lax.fori_loop(0, TD, tile, 0)


def prepare(vectors, staged, operand):
    count = len(vectors)
    height = operand.shape[1]
    pieces = [split3(v) for v in vectors]
    for k in range(3):
        for q in range(count):
            staged[pl.ds(k * count + q, EXT, stride=height), :] = pieces[q][k]
    for t in range(EXT):
        operand[t] = staged[t * height : (t + 1) * height, :].astype(BF16)


def weigh(listed, near, forces, operand, result, count, tiles):
    height = operand.shape[1]
    listed.wait()
    for k, s in enumerate(tiles):
        row = jnp.concatenate([operand[near[0, LIST + n * TD + s]] for n in range(NB)], axis=1)
        got = jnp.dot(row, forces[s], preferred_element_type=F32)
        result[k * height : (k + 1) * height, :] = got[:, TILE:] + got[:, :TILE]
    sums = []
    for q in range(count):
        parts = [result[pl.ds(k * count + q, len(tiles), stride=height), :] for k in (2, 1, 0)]
        sums.append(parts[0] + parts[1] + parts[2])
    return sums


def start_list(table, near, sem):
    listed = pltpu.make_async_copy(table, near, sem)
    listed.start()
    return listed


def limit(got, base, x, e, kappa, rho):
    square = jnp.zeros(e.shape, F32)
    for f in range(3):
        grad = (got[1 + f] - x[f] * got[0]) - e * (base[1 + f] - x[f] * base[0])
        square = square + grad * grad
    thick = kappa * rho
    ratio = jnp.sqrt(square) / (thick * e)
    return (2.0 + ratio) / ((6.0 + 3.0 * ratio + ratio * ratio) * thick)


INNER = range(HALF)
EDGE = range(HALF, TD)


def limiter_part(tiles, begin, listed, near, arranged, ext, forces, rho, e, fixed, operand, result, diff, sums):
    rows = slice(tiles[0], tiles[-1] + 1)
    got = weigh(listed, near, forces, operand, result, 8 if begin else 4, tiles)
    if begin:
        for q in range(4):
            fixed[q] = got[4 + q]
    base = [fixed[q] for q in range(4)]
    x = [ext[f, rows] - 0.5 for f in range(3)]
    value = limit(got, base, x, e[rows], arranged[6, rows], rho[rows])
    diff[...] = value
    sums[0] = base[0]
    sums[1] = got[0]
    return value


def limiter_edge(begin, *refs):
    *refs, staged, result, near, sem = refs
    listed = start_list(refs[1], near, sem)
    if begin:
        (mem, _, arranged, ext, forces, dens, d1, d2) = refs[:8]
        (diff, out1, out2, sums, operand, fixed, dens_ext) = refs[8:]
        odd = mem[0] % 2 == 1
        rho = extend(odd, dens[...], d1[...], d2[...])
        dens_ext[...] = rho
        e = ext[5]
    else:
        (mem, _, arranged, ext, forces, dens_ext, fixed, e_inner, e_edge, e1, e2) = refs[:11]
        (diff, out1, out2, sums, operand, e_ext) = refs[11:]
        odd = mem[0] % 2 == 1
        rho = dens_ext[...]
        e = extend(odd, jnp.concatenate([e_inner[...], e_edge[...]], axis=0), e1[...], e2[...])
        e_ext[...] = e
    v = (160.0 * KERNEL_NORM) * ext[3] / rho
    x = [ext[f] - 0.5 for f in range(3)]
    ve = v * e
    vectors = [ve] + [ve * x[f] for f in range(3)]
    if begin:
        vectors = vectors + [v] + [v * x[f] for f in range(3)]
    prepare(vectors, staged, operand)
    value = limiter_part(
        EDGE, begin, listed, near, arranged, ext, forces, rho, e, fixed, operand, result, diff, sums
    )
    send_parts(odd, value, out1, out2)


def limiter_inner(begin, *refs):
    *refs, result, near, sem = refs
    listed = start_list(refs[0], near, sem)
    (_, arranged, ext, forces, rho, e_ext, operand) = refs[:7]
    if begin:
        diff, sums, fixed = refs[7:]
        e = e_ext[5]
    else:
        fixed, diff, sums = refs[7:]
        e = e_ext[...]
    limiter_part(
        INNER, begin, listed, near, arranged, ext, forces, rho, e, fixed, operand, result, diff, sums
    )


def step_energy(arranged, rows, rho, sums, own, got):
    scale = TIME_STEP / rho[rows]
    rate = scale * (own * sums[0] + got[0])
    inflow = scale * (own * sums[1] + got[1])
    return (arranged[5, rows] + TIME_STEP * arranged[7, rows] + inflow) / (1.0 + rate)


def jacobi_edge(last, *refs):
    *refs, staged, result, near, sem = refs
    listed = start_list(refs[1], near, sem)
    (mem, _, arranged, ext, forces, rho, e_ext, inner_sums, sums, inner, edge, d1, d2) = refs[:13]
    odd = mem[0] % 2 == 1
    own = jnp.concatenate([inner[...], edge[...]], axis=0)
    spread = extend(odd, own, d1[...], d2[...])
    vd = ((160.0 * KERNEL_NORM) * ext[3] / rho[...]) * spread
    e = e_ext[5] if len(e_ext.shape) == 3 else e_ext[...]
    if last:
        dens, done, operand = refs[13:]
    else:
        new, out1, out2, operand = refs[13:]
    prepare([vd, vd * e], staged, operand)
    if last:
        got = weigh(listed, near, forces, operand, result, 2, range(TD))
        both = [jnp.concatenate([inner_sums[q], sums[q]], axis=0) for q in range(2)]
        value = step_energy(arranged, slice(0, TD), rho, both, own, got)
        for k, v in enumerate((value, dens[...])):
            done[k * TD : k * TD + GMAX] = v[HALF : HALF + GMAX]
            done[k * TD + GMAX : k * TD + GMAX + HALF] = v[:HALF]
            done[k * TD + GMAX + HALF : (k + 1) * TD] = v[HALF + GMAX :]
    else:
        got = weigh(listed, near, forces, operand, result, 2, EDGE)
        value = step_energy(arranged, slice(HALF, TD), rho, sums, edge[...], got)
        new[...] = value
        send_parts(odd, value, out1, out2)


def jacobi_inner(table, arranged, forces, rho, operand, sums, inner, new, result, near, sem):
    listed = start_list(table, near, sem)
    got = weigh(listed, near, forces, operand, result, 2, INNER)
    new[...] = step_energy(arranged, slice(0, HALF), rho, sums, inner[...], got)


def workspace(height, tiles, staged):
    stage = [pltpu.VMEM((EXT * height, TILE), F32)] if staged else []
    return stage + [pltpu.VMEM((tiles * height, TILE), F32), *LISTED]


def swap(first, second):
    odd = [(owner(s), owner(s + 1)) for s in range(1, GROUPS * 8 - 1, 2)]
    even = [(owner(s), owner(s + 1)) for s in range(0, GROUPS * 8 - 1, 2)]
    got = []
    for value, pairs in ((first, even), (second, odd)):
        got.append(lax.ppermute(value, AXES, pairs + [(b, a) for a, b in pairs]))
    return got


def local(particles, new_slot, neighbours, ghosts):
    grp, mem = [lax.axis_index(axis).astype(jnp.int32).reshape(1) for axis in AXES]
    hbm = pl.BlockSpec(memory_space=pltpu.MemorySpace.HBM)
    outgoing = pl.pallas_call(
        pack_body,
        out_shape=jax.ShapeDtypeStruct((GROUPS * ROWS, TILE), F32),
        in_specs=[
            pl.BlockSpec(memory_space=SMEM),
            pl.BlockSpec(memory_space=SMEM),
            hbm,
            hbm,
            hbm,
            hbm,
        ],
        out_specs=pl.BlockSpec(memory_space=VMEM),
        scratch_shapes=[
            pltpu.SMEM((GROUPS,), jnp.int32),
            pltpu.SMEM((1, 2), jnp.int32),
            pltpu.SMEM((TD,), jnp.int32),
            pltpu.VMEM((NB, TD), jnp.int32),
            pltpu.VMEM((8, TD * TILE), F32),
            pltpu.SemaphoreType.DMA((4,)),
        ],
        name="pack",
        compiler_params=pltpu.CompilerParams(vmem_limit_bytes=VMEM_LIMIT),
    )(
        grp,
        mem,
        *(
            pltpu.with_memory_space_constraint(a, pltpu.MemorySpace.HBM)
            for a in (ghosts, new_slot, neighbours.T, particles)
        ),
    )
    received = lax.all_to_all(
        outgoing.reshape(GROUPS * ROWS, 1, TILE), "group", split_axis=0, concat_axis=0, tiled=True
    )
    edge = ((GMAX, TILE), F32)
    own = ((TD, TILE), F32)
    wide = ((EXT, TILE), F32)
    arranged, s1, s2, near = call(
        unpack_body,
        [
            ((8, TD, TILE), F32),
            ((6, GMAX, TILE), F32),
            ((6, GMAX, TILE), F32),
            ((1, TILE), jnp.int32),
        ],
        [],
        "unpack",
        grp,
        mem,
        received.reshape(GROUPS * ROWS, TILE),
    )
    table = (mem, near)
    s1, s2 = swap(s1, s2)
    (cols,) = call(columns_body, [((5, EXT, TILE, TILE), F32)], [], "columns", arranged)
    density, ext, dist, r1, r2, cols = call(
        density_body,
        [
            own,
            ((6, EXT, TILE), F32),
            ((TD, NB * TILE, TILE), F32),
            edge,
            edge,
            ((5, EXT, TILE, TILE), F32),
        ],
        LISTED,
        "density",
        *table,
        arranged,
        s1,
        s2,
        cols,
        alias={5: 5},
    )
    r1, r2 = swap(r1, r2)
    (forces,) = call(
        forces_body,
        [((TD, NB * TILE, 2 * TILE), BF16)],
        LISTED,
        "forces",
        near,
        arranged,
        cols,
        dist,
    )
    shared = (*table, arranged, ext, forces)
    half = ((HALF, TILE), F32)
    pair = ((2, HALF, TILE), F32)
    four = ((4, HALF, TILE), F32)
    for step in range(SWEEPS):
        begin = step == 0
        height = 24 if begin else 16
        operand = ((EXT, height, TILE), BF16)
        if begin:
            diff, d1, d2, sums, rows, fixed, dens_ext = call(
                lambda *refs: limiter_edge(True, *refs),
                [half, edge, edge, pair, operand, four, wide],
                workspace(height, HALF, True),
                "limiter_first_edge",
                *shared,
                density,
                r1,
                r2,
            )
            e_ext = ext
        else:
            diff, d1, d2, sums, rows, e_ext = call(
                lambda *refs: limiter_edge(False, *refs),
                [half, edge, edge, pair, operand, wide],
                workspace(height, HALF, True),
                "limiter_edge",
                *shared,
                dens_ext,
                fixed,
                e_inner,
                e_edge,
                e1,
                e2,
            )
        d1, d2 = swap(d1, d2)
        results = call(
            lambda *refs: limiter_inner(begin, *refs),
            [half, pair, four] if begin else [half, pair],
            workspace(height, HALF, False),
            "limiter_first_inner" if begin else "limiter_inner",
            near,
            arranged,
            ext,
            forces,
            dens_ext,
            e_ext,
            rows,
            *(() if begin else (inner_fixed,)),
        )
        if begin:
            inner_diff, inner_sums, inner_fixed = results
        else:
            inner_diff, inner_sums = results
        last = step == SWEEPS - 1
        operand = ((EXT, 8, TILE), BF16)
        results = call(
            lambda *refs: jacobi_edge(last, *refs),
            [((2 * TD, TILE), F32), operand] if last else [half, edge, edge, operand],
            workspace(8, TD if last else HALF, True),
            "jacobi_last" if last else "jacobi_edge",
            *shared,
            dens_ext,
            e_ext,
            inner_sums,
            sums,
            inner_diff,
            diff,
            d1,
            d2,
            *((density,) if last else ()),
        )
        if last:
            done = results[0]
        else:
            e_edge, e1, e2, rows = results
            e1, e2 = swap(e1, e2)
            (e_inner,) = call(
                jacobi_inner,
                [half],
                workspace(8, HALF, False),
                "jacobi_inner",
                near,
                arranged,
                forces,
                dens_ext,
                rows,
                inner_sums,
                inner_diff,
            )
    done = lax.ppermute(done, AXES, [(owner(s), s) for s in range(GROUPS * 8)])
    return (done[:TD].reshape(-1), done[TD:].reshape(-1))


def solution(mesh):
    in_specs = (
        P(None, ("group", "member")),
        P(("group", "member")),
        P(("group", "member"), None),
        P(("group", "member"), None),
    )
    out_specs = (P(("group", "member")), P(("group", "member")))
    return jax.shard_map(local, mesh=mesh, in_specs=in_specs, out_specs=out_specs, check_vma=False)
```

```python
import math

import jax
import jax.numpy as jnp
from jax import lax
from jax.experimental import pallas as pl
from jax.experimental.pallas import tpu as pltpu
from jax.sharding import PartitionSpec as P

TILE = 128
GMAX = 4
SWEEPS = 3
NB = 6
TD = 16
EXT = TD + 2 * GMAX
ROWS = 17
GROUPS = 32
DEPTH = 8
LIST = 32
HALF = TD // 2
CHUNK = 32
KERNEL_NORM = 21.0 / (16.0 * math.pi)
TIME_STEP = 0.05
VMEM_LIMIT = 8 * 1024 * 1024
F32 = jnp.float32
BF16 = jnp.bfloat16
VMEM = pltpu.MemorySpace.VMEM
SMEM = pltpu.MemorySpace.SMEM
AXES = ("group", "member")


def call(body, outs, scratch, name, *args, alias={}):
    specs = [
        pl.BlockSpec(memory_space=SMEM if a.shape == (1,) else VMEM) for a in args
    ]
    return pl.pallas_call(
        body,
        out_shape=[jax.ShapeDtypeStruct(shape, dtype) for shape, dtype in outs],
        in_specs=specs,
        out_specs=[pl.BlockSpec(memory_space=VMEM) for _ in outs],
        scratch_shapes=scratch,
        name=name,
        input_output_aliases=alias,
        compiler_params=pltpu.CompilerParams(vmem_limit_bytes=VMEM_LIMIT),
    )(*args)


def owner(segment):
    group, member = divmod(segment, 8)
    if member in (5, 6):
        group = group // DEPTH * DEPTH + (group + 1) % DEPTH
    elif member == 7:
        group = (group + 1) % GROUPS
    return group * 8 + member


def moved_group(group, member):
    along = (group // DEPTH) * DEPTH + (group + 1) % DEPTH
    return jnp.where(member < 5, group, jnp.where(member < 7, along, (group + 1) % GROUPS))


def home_group(group, member):
    along = (group // DEPTH) * DEPTH + (group + DEPTH - 1) % DEPTH
    far = (group + GROUPS - 1) % GROUPS
    return jnp.where(member < 5, group, jnp.where(member < 7, along, far))


def pack_body(grp, mem, ghosts_hbm, slot_hbm, near_hbm, part_hbm, out, count, ghosts, slot, near, part, sem):
    copies = [
        pltpu.make_async_copy(source, target, sem.at[k])
        for k, (source, target) in enumerate(
            [(ghosts_hbm, ghosts), (slot_hbm, slot), (near_hbm, near), (part_hbm, part)]
        )
    ]
    for copy in copies:
        copy.start()
    out[...] = jnp.zeros(out.shape, F32)
    for g in range(GROUPS):
        count[g] = 0
        out[g * ROWS + 16 : g * ROWS + 17, :] = jnp.full((1, TILE), -1.0, F32)
    lane = lax.broadcasted_iota(jnp.int32, (1, TILE), 1)
    m = mem[0]
    for copy in copies:
        copy.wait()
    place = place_of(near[...], ghosts[0, 0]).astype(F32)
    place = jnp.concatenate(
        [place[:, GMAX : GMAX + HALF], place[:, :GMAX], place[:, GMAX + HALF :]], axis=1
    )
    row = jnp.full((1, TILE), -1.0, F32)
    for n in range(NB):
        first = LIST + n * TD
        piece = jnp.concatenate([place[n : n + 1], jnp.zeros((1, TILE - TD), F32)], axis=1)
        row = jnp.where((lane >= first) & (lane < first + TD), pltpu.roll(piece, first, 1), row)
    out[pl.ds(moved_group(grp[0], m) * ROWS + 16, 1), :] = row
    for t in range(TD):
        s = slot[t]
        g = moved_group(s // (TD * 8), m)
        n = count[g]
        count[g] = n + 1
        base = g * ROWS
        for r in range(8):
            out[pl.ds(base + n * 8 + r, 1), :] = part[r : r + 1, t * TILE : (t + 1) * TILE]
        label = pl.ds(base + 16, 1)
        here = (lane >= n * TD) & (lane < n * TD + TD)
        out[label, :] = jnp.where(here, rank(s % TD).astype(F32), out[label, :])


def split3(x):
    hi = x.astype(BF16).astype(F32)
    rest = x - hi
    mid = rest.astype(BF16).astype(F32)
    return hi, mid, rest - mid


def send_parts(odd, values, first, second):
    n = values.shape[-2]
    tail = values[..., n - GMAX :, :]
    head = values[..., n - HALF : n - GMAX, :]
    first[...] = jnp.where(odd, head, tail)
    second[...] = jnp.where(odd, tail, head)


def extend(odd, values, first, second):
    left = jnp.where(odd, first, second)
    right = jnp.where(odd, second, first)
    return jnp.concatenate([values, left, right], axis=-2)


def unpack_body(grp, mem, got, arranged, first, second, table):
    groups = got.shape[0] // ROWS
    odd = mem[0] % 2 == 1
    lane = lax.broadcasted_iota(jnp.int32, (groups, TILE), 1).astype(F32)
    labels = got[pl.ds(16, groups, stride=ROWS), :]
    marks = [
        jnp.where(values == lane, 1.0, 0.0)
        for values in (labels, pltpu.roll(labels, TILE - TD, 1))
    ]
    marks.append(jnp.zeros((TILE - 2 * groups, TILE), F32))
    choose = jnp.concatenate(marks, axis=0).T[:TD, : 2 * groups].astype(BF16)
    for r in range(8):
        tiles = jnp.concatenate(
            [got[pl.ds(n * 8 + r, groups, stride=ROWS), :] for n in range(2)], axis=0
        )
        moved = sum(
            jnp.dot(choose, piece.astype(BF16), preferred_element_type=F32)
            for piece in split3(tiles)
        )
        arranged[r] = moved
    mine = pl.ds(home_group(grp[0], mem[0]) * ROWS + 16, 1)
    table[...] = got[mine, :].astype(jnp.int32)
    send_parts(odd, arranged[0:6], first, second)


def place_of(entry, left):
    j = entry - left
    return jnp.where(j < 0, j + TD + GMAX, jnp.where(j < TD, rank(j), j + GMAX))


def rank(tile):
    return jnp.where(tile < GMAX, tile + HALF, jnp.where(tile < GMAX + HALF, tile - GMAX, tile))


LISTED = [pltpu.SMEM((1, TILE), jnp.int32), pltpu.SemaphoreType.DMA]


def spread_columns(cols, fields, tiles, first):
    turned = jnp.concatenate(fields, axis=0).T
    for f in range(5):
        for t in range(tiles):
            at = f * tiles + t
            cols[f, first + t] = jnp.broadcast_to(turned[:, at : at + 1], (TILE, TILE))


def columns_body(arranged, cols):
    spread_columns(cols, [arranged[f] for f in range(5)], TD, 0)


def density_body(
    mem, table, arranged, first, second, held, dens, ext, dist, out1, out2, cols, near, sem
):
    listed = pltpu.make_async_copy(table, near, sem)
    listed.start()
    odd = mem[0] % 2 == 1
    whole = extend(odd, arranged[0:6], first[...], second[...])
    ext[...] = whole
    spread_columns(cols, [whole[f, TD:] for f in range(5)], 2 * GMAX, TD)
    listed.wait()

    def tile(s, carry):
        own = [arranged[f, pl.ds(s, 1), :] for f in range(5)]
        x_i, y_i, z_i, _, h_i = [jnp.broadcast_to(v, (CHUNK, TILE)) for v in own]
        pace = 2.0 / h_i
        total = jnp.zeros((CHUNK, TILE), F32)
        for n in range(NB):
            t = near[0, LIST + n * TD + s]
            for c in range(TILE // CHUNK):
                rows = pl.ds(c * CHUNK, CHUNK)
                dx = cols[0, t, rows, :] - x_i
                dy = cols[1, t, rows, :] - y_i
                dz = cols[2, t, rows, :] - z_i
                r2 = dx * dx + dy * dy + dz * dz
                r = r2 * lax.rsqrt(jnp.maximum(r2, 1e-30))
                dist[s, pl.ds(n * TILE + c * CHUNK, CHUNK), :] = r
                u = jnp.maximum(4.0 - r * pace, 0.0)
                u2 = u * u
                total = total + (cols[3, t, rows, :] * (5.0 - u)) * (u2 * u2)
        dens[pl.ds(s, 1), :] = jnp.sum(total, axis=0, keepdims=True)
        return carry

    lax.fori_loop(0, TD, tile, 0)
    h = arranged[4]
    density = (KERNEL_NORM / 256.0) * dens[...] / (h * h * h)
    dens[...] = density
    send_parts(odd, density, out1, out2)


def forces_body(table, arranged, cols, dist, forces, near, sem):
    listed = pltpu.make_async_copy(table, near, sem)
    listed.start()
    listed.wait()

    def tile(s, carry):
        h_i = jnp.broadcast_to(arranged[4, pl.ds(s, 1), :], (CHUNK, TILE))
        for n in range(NB):
            t = near[0, LIST + n * TD + s]
            for c in range(TILE // CHUNK):
                at = pl.ds(n * TILE + c * CHUNK, CHUNK)
                reach = cols[4, t, pl.ds(c * CHUNK, CHUNK), :] + h_i
                w = jnp.maximum(reach - dist[s, at, :], 0.0)
                p2 = reach * reach
                q = w / (p2 * p2)
                force = q * q * w
                high = force.astype(BF16)
                forces[s, 0, at, :] = high
                forces[s, 1, at, :] = (force - high.astype(F32)).astype(BF16)
        return carry

    lax.fori_loop(0, TD, tile, 0)


def prepare(vectors, staged, operand):
    count = len(vectors)
    height = operand.shape[1]
    pieces = [split3(v) for v in vectors]
    for k in range(3):
        for q in range(count):
            staged[pl.ds(k * count + q, EXT, stride=height), :] = pieces[q][k]
    for t in range(EXT):
        operand[t] = staged[t * height : (t + 1) * height, :].astype(BF16)


def weigh(listed, near, forces, operand, result, count, tiles):
    height = operand.shape[1]
    listed.wait()
    for k, s in enumerate(tiles):
        row = jnp.concatenate([operand[near[0, LIST + n * TD + s]] for n in range(NB)], axis=1)
        both = jnp.concatenate([forces[s, 0], forces[s, 1]], axis=1)
        got = jnp.dot(row, both, preferred_element_type=F32)
        result[k * height : (k + 1) * height, :] = got[:, TILE:] + got[:, :TILE]
    sums = []
    for q in range(count):
        parts = [result[pl.ds(k * count + q, len(tiles), stride=height), :] for k in (2, 1, 0)]
        sums.append(parts[0] + parts[1] + parts[2])
    return sums


def start_list(table, near, sem):
    listed = pltpu.make_async_copy(table, near, sem)
    listed.start()
    return listed


def limit(got, base, x, e, kappa, rho):
    square = jnp.zeros(e.shape, F32)
    for f in range(3):
        grad = (got[1 + f] - x[f] * got[0]) - e * (base[1 + f] - x[f] * base[0])
        square = square + grad * grad
    thick = kappa * rho
    ratio = jnp.sqrt(square) / (thick * e)
    return (2.0 + ratio) / ((6.0 + 3.0 * ratio + ratio * ratio) * thick)


INNER = range(HALF)
EDGE = range(HALF, TD)


def limiter_part(tiles, begin, listed, near, arranged, ext, forces, rho, e, fixed, operand, result, diff, sums):
    rows = slice(tiles[0], tiles[-1] + 1)
    got = weigh(listed, near, forces, operand, result, 8 if begin else 4, tiles)
    if begin:
        for q in range(4):
            fixed[q] = got[4 + q]
    base = [fixed[q] for q in range(4)]
    x = [ext[f, rows] - 0.5 for f in range(3)]
    value = limit(got, base, x, e[rows], arranged[6, rows], rho[rows])
    diff[...] = value
    sums[0] = base[0]
    sums[1] = got[0]
    return value


def limiter_edge(begin, *refs):
    *refs, staged, result, near, sem = refs
    listed = start_list(refs[1], near, sem)
    if begin:
        (mem, _, arranged, ext, forces, dens, d1, d2) = refs[:8]
        (diff, out1, out2, sums, operand, fixed, dens_ext) = refs[8:]
        odd = mem[0] % 2 == 1
        rho = extend(odd, dens[...], d1[...], d2[...])
        dens_ext[...] = rho
        e = ext[5]
    else:
        (mem, _, arranged, ext, forces, dens_ext, fixed, e_inner, e_edge, e1, e2) = refs[:11]
        (diff, out1, out2, sums, operand, e_ext) = refs[11:]
        odd = mem[0] % 2 == 1
        rho = dens_ext[...]
        e = extend(odd, jnp.concatenate([e_inner[...], e_edge[...]], axis=0), e1[...], e2[...])
        e_ext[...] = e
    v = (160.0 * KERNEL_NORM) * ext[3] / rho
    x = [ext[f] - 0.5 for f in range(3)]
    ve = v * e
    vectors = [ve] + [ve * x[f] for f in range(3)]
    if begin:
        vectors = vectors + [v] + [v * x[f] for f in range(3)]
    prepare(vectors, staged, operand)
    value = limiter_part(
        EDGE, begin, listed, near, arranged, ext, forces, rho, e, fixed, operand, result, diff, sums
    )
    send_parts(odd, value, out1, out2)


def limiter_inner(begin, *refs):
    *refs, result, near, sem = refs
    listed = start_list(refs[0], near, sem)
    (_, arranged, ext, forces, rho, e_ext, operand) = refs[:7]
    if begin:
        diff, sums, fixed = refs[7:]
        e = e_ext[5]
    else:
        fixed, diff, sums = refs[7:]
        e = e_ext[...]
    limiter_part(
        INNER, begin, listed, near, arranged, ext, forces, rho, e, fixed, operand, result, diff, sums
    )


def step_energy(arranged, rows, rho, sums, own, got):
    scale = TIME_STEP / rho[rows]
    rate = scale * (own * sums[0] + got[0])
    inflow = scale * (own * sums[1] + got[1])
    return (arranged[5, rows] + TIME_STEP * arranged[7, rows] + inflow) / (1.0 + rate)


def jacobi_edge(last, *refs):
    *refs, staged, result, near, sem = refs
    listed = start_list(refs[1], near, sem)
    (mem, _, arranged, ext, forces, rho, e_ext, inner_sums, sums, inner, edge, d1, d2) = refs[:13]
    odd = mem[0] % 2 == 1
    own = jnp.concatenate([inner[...], edge[...]], axis=0)
    spread = extend(odd, own, d1[...], d2[...])
    vd = ((160.0 * KERNEL_NORM) * ext[3] / rho[...]) * spread
    e = e_ext[5] if len(e_ext.shape) == 3 else e_ext[...]
    if last:
        dens, done, operand = refs[13:]
    else:
        new, out1, out2, operand = refs[13:]
    prepare([vd, vd * e], staged, operand)
    if last:
        got = weigh(listed, near, forces, operand, result, 2, range(TD))
        both = [jnp.concatenate([inner_sums[q], sums[q]], axis=0) for q in range(2)]
        value = step_energy(arranged, slice(0, TD), rho, both, own, got)
        for k, v in enumerate((value, dens[...])):
            done[k * TD : k * TD + GMAX] = v[HALF : HALF + GMAX]
            done[k * TD + GMAX : k * TD + GMAX + HALF] = v[:HALF]
            done[k * TD + GMAX + HALF : (k + 1) * TD] = v[HALF + GMAX :]
    else:
        got = weigh(listed, near, forces, operand, result, 2, EDGE)
        value = step_energy(arranged, slice(HALF, TD), rho, sums, edge[...], got)
        new[...] = value
        send_parts(odd, value, out1, out2)


def jacobi_inner(table, arranged, forces, rho, operand, sums, inner, new, result, near, sem):
    listed = start_list(table, near, sem)
    got = weigh(listed, near, forces, operand, result, 2, INNER)
    new[...] = step_energy(arranged, slice(0, HALF), rho, sums, inner[...], got)


def workspace(height, tiles, staged):
    stage = [pltpu.VMEM((EXT * height, TILE), F32)] if staged else []
    return stage + [pltpu.VMEM((tiles * height, TILE), F32), *LISTED]


def swap(first, second):
    odd = [(owner(s), owner(s + 1)) for s in range(1, GROUPS * 8 - 1, 2)]
    even = [(owner(s), owner(s + 1)) for s in range(0, GROUPS * 8 - 1, 2)]
    got = []
    for value, pairs in ((first, even), (second, odd)):
        got.append(lax.ppermute(value, AXES, pairs + [(b, a) for a, b in pairs]))
    return got


def local(particles, new_slot, neighbours, ghosts):
    grp, mem = [lax.axis_index(axis).astype(jnp.int32).reshape(1) for axis in AXES]
    hbm = pl.BlockSpec(memory_space=pltpu.MemorySpace.HBM)
    outgoing = pl.pallas_call(
        pack_body,
        out_shape=jax.ShapeDtypeStruct((GROUPS * ROWS, TILE), F32),
        in_specs=[
            pl.BlockSpec(memory_space=SMEM),
            pl.BlockSpec(memory_space=SMEM),
            hbm,
            hbm,
            hbm,
            hbm,
        ],
        out_specs=pl.BlockSpec(memory_space=VMEM),
        scratch_shapes=[
            pltpu.SMEM((GROUPS,), jnp.int32),
            pltpu.SMEM((1, 2), jnp.int32),
            pltpu.SMEM((TD,), jnp.int32),
            pltpu.VMEM((NB, TD), jnp.int32),
            pltpu.VMEM((8, TD * TILE), F32),
            pltpu.SemaphoreType.DMA((4,)),
        ],
        name="pack",
        compiler_params=pltpu.CompilerParams(vmem_limit_bytes=VMEM_LIMIT),
    )(
        grp,
        mem,
        *(
            pltpu.with_memory_space_constraint(a, pltpu.MemorySpace.HBM)
            for a in (ghosts, new_slot, neighbours.T, particles)
        ),
    )
    received = lax.all_to_all(
        outgoing.reshape(GROUPS * ROWS, 1, TILE), "group", split_axis=0, concat_axis=0, tiled=True
    )
    edge = ((GMAX, TILE), F32)
    own = ((TD, TILE), F32)
    wide = ((EXT, TILE), F32)
    arranged, s1, s2, near = call(
        unpack_body,
        [
            ((8, TD, TILE), F32),
            ((6, GMAX, TILE), F32),
            ((6, GMAX, TILE), F32),
            ((1, TILE), jnp.int32),
        ],
        [],
        "unpack",
        grp,
        mem,
        received.reshape(GROUPS * ROWS, TILE),
    )
    table = (mem, near)
    s1, s2 = swap(s1, s2)
    (cols,) = call(columns_body, [((5, EXT, TILE, TILE), F32)], [], "columns", arranged)
    density, ext, dist, r1, r2, cols = call(
        density_body,
        [
            own,
            ((6, EXT, TILE), F32),
            ((TD, NB * TILE, TILE), F32),
            edge,
            edge,
            ((5, EXT, TILE, TILE), F32),
        ],
        LISTED,
        "density",
        *table,
        arranged,
        s1,
        s2,
        cols,
        alias={5: 5},
    )
    r1, r2 = swap(r1, r2)
    (forces,) = call(
        forces_body,
        [((TD, 2, NB * TILE, TILE), BF16)],
        LISTED,
        "forces",
        near,
        arranged,
        cols,
        dist,
    )
    shared = (*table, arranged, ext, forces)
    half = ((HALF, TILE), F32)
    pair = ((2, HALF, TILE), F32)
    four = ((4, HALF, TILE), F32)
    for step in range(SWEEPS):
        begin = step == 0
        height = 24 if begin else 16
        operand = ((EXT, height, TILE), BF16)
        if begin:
            diff, d1, d2, sums, rows, fixed, dens_ext = call(
                lambda *refs: limiter_edge(True, *refs),
                [half, edge, edge, pair, operand, four, wide],
                workspace(height, HALF, True),
                "limiter_first_edge",
                *shared,
                density,
                r1,
                r2,
            )
            e_ext = ext
        else:
            diff, d1, d2, sums, rows, e_ext = call(
                lambda *refs: limiter_edge(False, *refs),
                [half, edge, edge, pair, operand, wide],
                workspace(height, HALF, True),
                "limiter_edge",
                *shared,
                dens_ext,
                fixed,
                e_inner,
                e_edge,
                e1,
                e2,
            )
        d1, d2 = swap(d1, d2)
        results = call(
            lambda *refs: limiter_inner(begin, *refs),
            [half, pair, four] if begin else [half, pair],
            workspace(height, HALF, False),
            "limiter_first_inner" if begin else "limiter_inner",
            near,
            arranged,
            ext,
            forces,
            dens_ext,
            e_ext,
            rows,
            *(() if begin else (inner_fixed,)),
        )
        if begin:
            inner_diff, inner_sums, inner_fixed = results
        else:
            inner_diff, inner_sums = results
        last = step == SWEEPS - 1
        operand = ((EXT, 8, TILE), BF16)
        results = call(
            lambda *refs: jacobi_edge(last, *refs),
            [((2 * TD, TILE), F32)] if last else [half, edge, edge, operand],
            ([pltpu.VMEM(*operand)] if last else []) + workspace(8, TD if last else HALF, True),
            "jacobi_last" if last else "jacobi_edge",
            *shared,
            dens_ext,
            e_ext,
            inner_sums,
            sums,
            inner_diff,
            diff,
            d1,
            d2,
            *((density,) if last else ()),
        )
        if last:
            done = results[0]
        else:
            e_edge, e1, e2, rows = results
            e1, e2 = swap(e1, e2)
            (e_inner,) = call(
                jacobi_inner,
                [half],
                workspace(8, HALF, False),
                "jacobi_inner",
                near,
                arranged,
                forces,
                dens_ext,
                rows,
                inner_sums,
                inner_diff,
            )
    done = lax.ppermute(done, AXES, [(owner(s), s) for s in range(GROUPS * 8)])
    return (done[:TD].reshape(-1), done[TD:].reshape(-1))


def solution(mesh):
    in_specs = (
        P(None, ("group", "member")),
        P(("group", "member")),
        P(("group", "member"), None),
        P(("group", "member"), None),
    )
    out_specs = (P(("group", "member")), P(("group", "member")))
    return jax.shard_map(local, mesh=mesh, in_specs=in_specs, out_specs=out_specs, check_vma=False)
```

```python
import math

import jax
import jax.numpy as jnp
from jax import lax
from jax.experimental import pallas as pl
from jax.experimental.pallas import tpu as pltpu
from jax.sharding import PartitionSpec as P

TILE = 128
GMAX = 4
SWEEPS = 3
NB = 6
TD = 16
EXT = TD + 2 * GMAX
ROWS = 17
GROUPS = 32
DEPTH = 8
LIST = 32
HALF = TD // 2
CHUNK = 32
KERNEL_NORM = 21.0 / (16.0 * math.pi)
TIME_STEP = 0.05
VMEM_LIMIT = 8 * 1024 * 1024
F32 = jnp.float32
BF16 = jnp.bfloat16
VMEM = pltpu.MemorySpace.VMEM
SMEM = pltpu.MemorySpace.SMEM
AXES = ("group", "member")


def call(body, outs, scratch, name, *args, alias={}):
    specs = [
        pl.BlockSpec(memory_space=SMEM if a.shape == (1,) else VMEM) for a in args
    ]
    return pl.pallas_call(
        body,
        out_shape=[jax.ShapeDtypeStruct(shape, dtype) for shape, dtype in outs],
        in_specs=specs,
        out_specs=[pl.BlockSpec(memory_space=VMEM) for _ in outs],
        scratch_shapes=scratch,
        name=name,
        input_output_aliases=alias,
        compiler_params=pltpu.CompilerParams(vmem_limit_bytes=VMEM_LIMIT),
    )(*args)


def owner(segment):
    group, member = divmod(segment, 8)
    if member in (5, 6):
        group = group // DEPTH * DEPTH + (group + 1) % DEPTH
    elif member == 7:
        group = (group + 1) % GROUPS
    return group * 8 + member


def moved_group(group, member):
    along = (group // DEPTH) * DEPTH + (group + 1) % DEPTH
    return jnp.where(member < 5, group, jnp.where(member < 7, along, (group + 1) % GROUPS))


def home_group(group, member):
    along = (group // DEPTH) * DEPTH + (group + DEPTH - 1) % DEPTH
    far = (group + GROUPS - 1) % GROUPS
    return jnp.where(member < 5, group, jnp.where(member < 7, along, far))


def pack_body(grp, mem, ghosts_hbm, slot_hbm, near_hbm, part_hbm, out, count, ghosts, slot, near, part, sem):
    copies = [
        pltpu.make_async_copy(source, target, sem.at[k])
        for k, (source, target) in enumerate(
            [(ghosts_hbm, ghosts), (slot_hbm, slot), (near_hbm, near), (part_hbm, part)]
        )
    ]
    for copy in copies:
        copy.start()
    out[...] = jnp.zeros(out.shape, F32)
    for g in range(GROUPS):
        count[g] = 0
        out[g * ROWS + 16 : g * ROWS + 17, :] = jnp.full((1, TILE), -1.0, F32)
    lane = lax.broadcasted_iota(jnp.int32, (1, TILE), 1)
    m = mem[0]
    for copy in copies:
        copy.wait()
    place = place_of(near[...], ghosts[0, 0]).astype(F32)
    place = jnp.concatenate(
        [place[:, GMAX : GMAX + HALF], place[:, :GMAX], place[:, GMAX + HALF :]], axis=1
    )
    row = jnp.full((1, TILE), -1.0, F32)
    for n in range(NB):
        first = LIST + n * TD
        piece = jnp.concatenate([place[n : n + 1], jnp.zeros((1, TILE - TD), F32)], axis=1)
        row = jnp.where((lane >= first) & (lane < first + TD), pltpu.roll(piece, first, 1), row)
    out[pl.ds(moved_group(grp[0], m) * ROWS + 16, 1), :] = row
    for t in range(TD):
        s = slot[t]
        g = moved_group(s // (TD * 8), m)
        n = count[g]
        count[g] = n + 1
        base = g * ROWS
        for r in range(8):
            out[pl.ds(base + n * 8 + r, 1), :] = part[r : r + 1, t * TILE : (t + 1) * TILE]
        label = pl.ds(base + 16, 1)
        here = (lane >= n * TD) & (lane < n * TD + TD)
        out[label, :] = jnp.where(here, rank(s % TD).astype(F32), out[label, :])


def split3(x):
    hi = x.astype(BF16).astype(F32)
    rest = x - hi
    mid = rest.astype(BF16).astype(F32)
    return hi, mid, rest - mid


def send_parts(odd, values, first, second):
    n = values.shape[-2]
    tail = values[..., n - GMAX :, :]
    head = values[..., n - HALF : n - GMAX, :]
    first[...] = jnp.where(odd, head, tail)
    second[...] = jnp.where(odd, tail, head)


def extend(odd, values, first, second):
    left = jnp.where(odd, first, second)
    right = jnp.where(odd, second, first)
    return jnp.concatenate([values, left, right], axis=-2)


def unpack_body(grp, mem, got, arranged, first, second, table):
    groups = got.shape[0] // ROWS
    odd = mem[0] % 2 == 1
    lane = lax.broadcasted_iota(jnp.int32, (groups, TILE), 1).astype(F32)
    labels = got[pl.ds(16, groups, stride=ROWS), :]
    marks = [
        jnp.where(values == lane, 1.0, 0.0)
        for values in (labels, pltpu.roll(labels, TILE - TD, 1))
    ]
    marks.append(jnp.zeros((TILE - 2 * groups, TILE), F32))
    choose = jnp.concatenate(marks, axis=0).T[:TD, : 2 * groups].astype(BF16)
    for r in range(8):
        tiles = jnp.concatenate(
            [got[pl.ds(n * 8 + r, groups, stride=ROWS), :] for n in range(2)], axis=0
        )
        moved = sum(
            jnp.dot(choose, piece.astype(BF16), preferred_element_type=F32)
            for piece in split3(tiles)
        )
        arranged[r] = moved
    mine = pl.ds(home_group(grp[0], mem[0]) * ROWS + 16, 1)
    table[...] = got[mine, :].astype(jnp.int32)
    send_parts(odd, arranged[0:6], first, second)


def place_of(entry, left):
    j = entry - left
    return jnp.where(j < 0, j + TD + GMAX, jnp.where(j < TD, rank(j), j + GMAX))


def rank(tile):
    return jnp.where(tile < GMAX, tile + HALF, jnp.where(tile < GMAX + HALF, tile - GMAX, tile))


LISTED = [pltpu.SMEM((1, TILE), jnp.int32), pltpu.SemaphoreType.DMA]


def spread_columns(cols, fields, tiles, first):
    turned = jnp.concatenate(fields, axis=0).T
    for f in range(5):
        for t in range(tiles):
            at = f * tiles + t
            cols[f, first + t] = jnp.broadcast_to(turned[:, at : at + 1], (TILE, TILE))


def columns_body(arranged, cols):
    spread_columns(cols, [arranged[f] for f in range(5)], TD, 0)


def density_edge(
    mem, table, arranged, first, second, held, dens, ext, dist, out1, out2, cols, near, sem
):
    listed = start_list(table, near, sem)
    odd = mem[0] % 2 == 1
    whole = extend(odd, arranged[0:6], first[...], second[...])
    ext[...] = whole
    spread_columns(cols, [whole[f, TD:] for f in range(5)], 2 * GMAX, TD)
    listed.wait()
    send_parts(odd, find_density(HALF, near, arranged, cols, dens, dist), out1, out2)


def density_inner(table, arranged, cols, dens, dist, near, sem):
    start_list(table, near, sem).wait()
    find_density(0, near, arranged, cols, dens, dist)


def find_density(begin, near, arranged, cols, dens, dist):
    def tile(k, carry):
        s = begin + k
        own = [arranged[f, pl.ds(s, 1), :] for f in range(5)]
        x_i, y_i, z_i, _, h_i = [jnp.broadcast_to(v, (CHUNK, TILE)) for v in own]
        pace = 2.0 / h_i
        total = jnp.zeros((CHUNK, TILE), F32)
        for n in range(NB):
            t = near[0, LIST + n * TD + s]
            for c in range(TILE // CHUNK):
                rows = pl.ds(c * CHUNK, CHUNK)
                dx = cols[0, t, rows, :] - x_i
                dy = cols[1, t, rows, :] - y_i
                dz = cols[2, t, rows, :] - z_i
                r2 = dx * dx + dy * dy + dz * dz
                r = r2 * lax.rsqrt(jnp.maximum(r2, 1e-30))
                dist[k, pl.ds(n * TILE + c * CHUNK, CHUNK), :] = r
                u = jnp.maximum(4.0 - r * pace, 0.0)
                u2 = u * u
                total = total + (cols[3, t, rows, :] * (5.0 - u)) * (u2 * u2)
        dens[pl.ds(k, 1), :] = jnp.sum(total, axis=0, keepdims=True)
        return carry

    lax.fori_loop(0, HALF, tile, 0)
    h = arranged[4, begin : begin + HALF]
    density = (KERNEL_NORM / 256.0) * dens[...] / (h * h * h)
    dens[...] = density
    return density


def forces_body(begin, table, arranged, cols, dist, *refs):
    *_, forces, near, sem = refs
    start_list(table, near, sem).wait()

    def tile(k, carry):
        s = begin + k
        h_i = jnp.broadcast_to(arranged[4, pl.ds(s, 1), :], (CHUNK, TILE))
        for n in range(NB):
            t = near[0, LIST + n * TD + s]
            for c in range(TILE // CHUNK):
                at = pl.ds(n * TILE + c * CHUNK, CHUNK)
                reach = cols[4, t, pl.ds(c * CHUNK, CHUNK), :] + h_i
                w = jnp.maximum(reach - dist[k, at, :], 0.0)
                p2 = reach * reach
                q = w / (p2 * p2)
                force = q * q * w
                high = force.astype(BF16)
                forces[k, 0, at, :] = high
                forces[k, 1, at, :] = (force - high.astype(F32)).astype(BF16)
        return carry

    lax.fori_loop(0, HALF, tile, 0)


def prepare(vectors, staged, operand):
    count = len(vectors)
    height = operand.shape[1]
    pieces = [split3(v) for v in vectors]
    for k in range(3):
        for q in range(count):
            staged[pl.ds(k * count + q, EXT, stride=height), :] = pieces[q][k]
    for t in range(EXT):
        operand[t] = staged[t * height : (t + 1) * height, :].astype(BF16)


def weigh(listed, near, forces, operand, result, count, tiles):
    height = operand.shape[1]
    listed.wait()
    for k, s in enumerate(tiles):
        row = jnp.concatenate([operand[near[0, LIST + n * TD + s]] for n in range(NB)], axis=1)
        block = forces[k // HALF] if isinstance(forces, tuple) else forces
        both = jnp.concatenate([block[k % HALF, 0], block[k % HALF, 1]], axis=1)
        got = jnp.dot(row, both, preferred_element_type=F32)
        result[k * height : (k + 1) * height, :] = got[:, TILE:] + got[:, :TILE]
    sums = []
    for q in range(count):
        parts = [result[pl.ds(k * count + q, len(tiles), stride=height), :] for k in (2, 1, 0)]
        sums.append(parts[0] + parts[1] + parts[2])
    return sums


def start_list(table, near, sem):
    listed = pltpu.make_async_copy(table, near, sem)
    listed.start()
    return listed


def limit(got, base, x, e, kappa, rho):
    square = jnp.zeros(e.shape, F32)
    for f in range(3):
        grad = (got[1 + f] - x[f] * got[0]) - e * (base[1 + f] - x[f] * base[0])
        square = square + grad * grad
    thick = kappa * rho
    ratio = jnp.sqrt(square) / (thick * e)
    return (2.0 + ratio) / ((6.0 + 3.0 * ratio + ratio * ratio) * thick)


INNER = range(HALF)
EDGE = range(HALF, TD)


def limiter_part(tiles, begin, listed, near, arranged, ext, forces, rho, e, fixed, operand, result, diff, sums):
    rows = slice(tiles[0], tiles[-1] + 1)
    got = weigh(listed, near, forces, operand, result, 8 if begin else 4, tiles)
    if begin:
        for q in range(4):
            fixed[q] = got[4 + q]
    base = [fixed[q] for q in range(4)]
    x = [ext[f, rows] - 0.5 for f in range(3)]
    value = limit(got, base, x, e[rows], arranged[6, rows], rho[rows])
    diff[...] = value
    sums[0] = base[0]
    sums[1] = got[0]
    return value


def limiter_edge(begin, *refs):
    *refs, staged, result, near, sem = refs
    listed = start_list(refs[1], near, sem)
    if begin:
        (mem, _, arranged, ext, forces, dens_inner, dens, d1, d2) = refs[:9]
        (diff, out1, out2, sums, operand, fixed, dens_ext) = refs[9:]
        odd = mem[0] % 2 == 1
        rho = extend(odd, jnp.concatenate([dens_inner[...], dens[...]], axis=0), d1[...], d2[...])
        dens_ext[...] = rho
        e = ext[5]
    else:
        (mem, _, arranged, ext, forces, dens_ext, fixed, e_inner, e_edge, e1, e2) = refs[:11]
        (diff, out1, out2, sums, operand, e_ext) = refs[11:]
        odd = mem[0] % 2 == 1
        rho = dens_ext[...]
        e = extend(odd, jnp.concatenate([e_inner[...], e_edge[...]], axis=0), e1[...], e2[...])
        e_ext[...] = e
    v = (160.0 * KERNEL_NORM) * ext[3] / rho
    x = [ext[f] - 0.5 for f in range(3)]
    ve = v * e
    vectors = [ve] + [ve * x[f] for f in range(3)]
    if begin:
        vectors = vectors + [v] + [v * x[f] for f in range(3)]
    prepare(vectors, staged, operand)
    value = limiter_part(
        EDGE, begin, listed, near, arranged, ext, forces, rho, e, fixed, operand, result, diff, sums
    )
    send_parts(odd, value, out1, out2)


def limiter_inner(begin, *refs):
    *refs, result, near, sem = refs
    listed = start_list(refs[0], near, sem)
    (_, arranged, ext, forces, rho, e_ext, operand) = refs[:7]
    if begin:
        diff, sums, fixed = refs[7:]
        e = e_ext[5]
    else:
        fixed, diff, sums = refs[7:]
        e = e_ext[...]
    limiter_part(
        INNER, begin, listed, near, arranged, ext, forces, rho, e, fixed, operand, result, diff, sums
    )


def step_energy(arranged, rows, rho, sums, own, got):
    scale = TIME_STEP / rho[rows]
    rate = scale * (own * sums[0] + got[0])
    inflow = scale * (own * sums[1] + got[1])
    return (arranged[5, rows] + TIME_STEP * arranged[7, rows] + inflow) / (1.0 + rate)


def jacobi_edge(last, *refs):
    *refs, staged, result, near, sem = refs
    listed = start_list(refs[1], near, sem)
    (mem, _, arranged, ext, forces, rho, e_ext, inner_sums, sums, inner, edge, d1, d2) = refs[:13]
    odd = mem[0] % 2 == 1
    own = jnp.concatenate([inner[...], edge[...]], axis=0)
    spread = extend(odd, own, d1[...], d2[...])
    vd = ((160.0 * KERNEL_NORM) * ext[3] / rho[...]) * spread
    e = e_ext[5] if len(e_ext.shape) == 3 else e_ext[...]
    if last:
        inner_forces, done, operand = refs[13:]
    else:
        new, out1, out2, operand = refs[13:]
    prepare([vd, vd * e], staged, operand)
    if last:
        got = weigh(listed, near, (inner_forces, forces), operand, result, 2, range(TD))
        both = [jnp.concatenate([inner_sums[q], sums[q]], axis=0) for q in range(2)]
        value = step_energy(arranged, slice(0, TD), rho, both, own, got)
        for k, v in enumerate((value, rho[:TD])):
            done[k * TD : k * TD + GMAX] = v[HALF : HALF + GMAX]
            done[k * TD + GMAX : k * TD + GMAX + HALF] = v[:HALF]
            done[k * TD + GMAX + HALF : (k + 1) * TD] = v[HALF + GMAX :]
    else:
        got = weigh(listed, near, forces, operand, result, 2, EDGE)
        value = step_energy(arranged, slice(HALF, TD), rho, sums, edge[...], got)
        new[...] = value
        send_parts(odd, value, out1, out2)


def jacobi_inner(table, arranged, forces, rho, operand, sums, inner, new, result, near, sem):
    listed = start_list(table, near, sem)
    got = weigh(listed, near, forces, operand, result, 2, INNER)
    new[...] = step_energy(arranged, slice(0, HALF), rho, sums, inner[...], got)


def workspace(height, tiles, staged):
    stage = [pltpu.VMEM((EXT * height, TILE), F32)] if staged else []
    return stage + [pltpu.VMEM((tiles * height, TILE), F32), *LISTED]


def swap(first, second):
    odd = [(owner(s), owner(s + 1)) for s in range(1, GROUPS * 8 - 1, 2)]
    even = [(owner(s), owner(s + 1)) for s in range(0, GROUPS * 8 - 1, 2)]
    got = []
    for value, pairs in ((first, even), (second, odd)):
        got.append(lax.ppermute(value, AXES, pairs + [(b, a) for a, b in pairs]))
    return got


def local(particles, new_slot, neighbours, ghosts):
    grp, mem = [lax.axis_index(axis).astype(jnp.int32).reshape(1) for axis in AXES]
    hbm = pl.BlockSpec(memory_space=pltpu.MemorySpace.HBM)
    outgoing = pl.pallas_call(
        pack_body,
        out_shape=jax.ShapeDtypeStruct((GROUPS * ROWS, TILE), F32),
        in_specs=[
            pl.BlockSpec(memory_space=SMEM),
            pl.BlockSpec(memory_space=SMEM),
            hbm,
            hbm,
            hbm,
            hbm,
        ],
        out_specs=pl.BlockSpec(memory_space=VMEM),
        scratch_shapes=[
            pltpu.SMEM((GROUPS,), jnp.int32),
            pltpu.SMEM((1, 2), jnp.int32),
            pltpu.SMEM((TD,), jnp.int32),
            pltpu.VMEM((NB, TD), jnp.int32),
            pltpu.VMEM((8, TD * TILE), F32),
            pltpu.SemaphoreType.DMA((4,)),
        ],
        name="pack",
        compiler_params=pltpu.CompilerParams(vmem_limit_bytes=VMEM_LIMIT),
    )(
        grp,
        mem,
        *(
            pltpu.with_memory_space_constraint(a, pltpu.MemorySpace.HBM)
            for a in (ghosts, new_slot, neighbours.T, particles)
        ),
    )
    received = lax.all_to_all(
        outgoing.reshape(GROUPS * ROWS, 1, TILE), "group", split_axis=0, concat_axis=0, tiled=True
    )
    edge = ((GMAX, TILE), F32)
    own = ((TD, TILE), F32)
    wide = ((EXT, TILE), F32)
    arranged, s1, s2, near = call(
        unpack_body,
        [
            ((8, TD, TILE), F32),
            ((6, GMAX, TILE), F32),
            ((6, GMAX, TILE), F32),
            ((1, TILE), jnp.int32),
        ],
        [],
        "unpack",
        grp,
        mem,
        received.reshape(GROUPS * ROWS, TILE),
    )
    table = (mem, near)
    s1, s2 = swap(s1, s2)
    (cols,) = call(columns_body, [((5, EXT, TILE, TILE), F32)], [], "columns", arranged)
    half = ((HALF, TILE), F32)
    apart = ((HALF, NB * TILE, TILE), F32)
    block = ((HALF, 2, NB * TILE, TILE), BF16)
    dens, ext, dist, r1, r2, cols = call(
        density_edge,
        [half, ((6, EXT, TILE), F32), apart, edge, edge, ((5, EXT, TILE, TILE), F32)],
        LISTED,
        "density_edge",
        *table,
        arranged,
        s1,
        s2,
        cols,
        alias={5: 5},
    )
    r1, r2 = swap(r1, r2)
    dens_inner, inner_dist = call(
        density_inner, [half, apart], LISTED, "density_inner", near, arranged, cols
    )
    (forces,) = call(
        lambda *refs: forces_body(HALF, *refs),
        [block],
        LISTED,
        "forces_edge",
        near,
        arranged,
        cols,
        dist,
    )
    shared = (*table, arranged, ext, forces)
    pair = ((2, HALF, TILE), F32)
    four = ((4, HALF, TILE), F32)
    for step in range(SWEEPS):
        begin = step == 0
        height = 24 if begin else 16
        operand = ((EXT, height, TILE), BF16)
        if begin:
            diff, d1, d2, sums, rows, fixed, dens_ext = call(
                lambda *refs: limiter_edge(True, *refs),
                [half, edge, edge, pair, operand, four, wide],
                workspace(height, HALF, True),
                "limiter_first_edge",
                *shared,
                dens_inner,
                dens,
                r1,
                r2,
            )
            e_ext = ext
        else:
            diff, d1, d2, sums, rows, e_ext = call(
                lambda *refs: limiter_edge(False, *refs),
                [half, edge, edge, pair, operand, wide],
                workspace(height, HALF, True),
                "limiter_edge",
                *shared,
                dens_ext,
                fixed,
                e_inner,
                e_edge,
                e1,
                e2,
            )
        d1, d2 = swap(d1, d2)
        if begin:
            (inner_forces,) = call(
                lambda *refs: forces_body(0, *refs),
                [block],
                LISTED,
                "forces_inner",
                near,
                arranged,
                cols,
                inner_dist,
                diff,
            )
        results = call(
            lambda *refs: limiter_inner(begin, *refs),
            [half, pair, four] if begin else [half, pair],
            workspace(height, HALF, False),
            "limiter_first_inner" if begin else "limiter_inner",
            near,
            arranged,
            ext,
            inner_forces,
            dens_ext,
            e_ext,
            rows,
            *(() if begin else (inner_fixed,)),
        )
        if begin:
            inner_diff, inner_sums, inner_fixed = results
        else:
            inner_diff, inner_sums = results
        last = step == SWEEPS - 1
        operand = ((EXT, 8, TILE), BF16)
        results = call(
            lambda *refs: jacobi_edge(last, *refs),
            [((2 * TD, TILE), F32)] if last else [half, edge, edge, operand],
            ([pltpu.VMEM(*operand)] if last else []) + workspace(8, TD if last else HALF, True),
            "jacobi_last" if last else "jacobi_edge",
            *shared,
            dens_ext,
            e_ext,
            inner_sums,
            sums,
            inner_diff,
            diff,
            d1,
            d2,
            *((inner_forces,) if last else ()),
        )
        if last:
            done = results[0]
        else:
            e_edge, e1, e2, rows = results
            e1, e2 = swap(e1, e2)
            (e_inner,) = call(
                jacobi_inner,
                [half],
                workspace(8, HALF, False),
                "jacobi_inner",
                near,
                arranged,
                inner_forces,
                dens_ext,
                rows,
                inner_sums,
                inner_diff,
            )
    done = lax.ppermute(done, AXES, [(owner(s), s) for s in range(GROUPS * 8)])
    return (done[:TD].reshape(-1), done[TD:].reshape(-1))


def solution(mesh):
    in_specs = (
        P(None, ("group", "member")),
        P(("group", "member")),
        P(("group", "member"), None),
        P(("group", "member"), None),
    )
    out_specs = (P(("group", "member")), P(("group", "member")))
    return jax.shard_map(local, mesh=mesh, in_specs=in_specs, out_specs=out_specs, check_vma=False)
```

```python
import math

import jax
import jax.numpy as jnp
from jax import lax
from jax.experimental import pallas as pl
from jax.experimental.pallas import tpu as pltpu
from jax.sharding import PartitionSpec as P

TILE = 128
GMAX = 4
SWEEPS = 3
NB = 6
TD = 16
EXT = TD + 2 * GMAX
ROWS = 17
GROUPS = 32
DEPTH = 8
LIST = 32
HALF = TD // 2
CHUNK = 32
KERNEL_NORM = 21.0 / (16.0 * math.pi)
TIME_STEP = 0.05
VMEM_LIMIT = 8 * 1024 * 1024
F32 = jnp.float32
BF16 = jnp.bfloat16
VMEM = pltpu.MemorySpace.VMEM
SMEM = pltpu.MemorySpace.SMEM
AXES = ("group", "member")


def call(body, outs, scratch, name, *args, alias={}):
    specs = [
        pl.BlockSpec(memory_space=SMEM if a.shape == (1,) else VMEM) for a in args
    ]
    return pl.pallas_call(
        body,
        out_shape=[jax.ShapeDtypeStruct(shape, dtype) for shape, dtype in outs],
        in_specs=specs,
        out_specs=[pl.BlockSpec(memory_space=VMEM) for _ in outs],
        scratch_shapes=scratch,
        name=name,
        input_output_aliases=alias,
        compiler_params=pltpu.CompilerParams(vmem_limit_bytes=VMEM_LIMIT),
    )(*args)


def owner(segment):
    group, member = divmod(segment, 8)
    if member in (5, 6):
        group = group // DEPTH * DEPTH + (group + 1) % DEPTH
    elif member == 7:
        group = (group + 1) % GROUPS
    return group * 8 + member


def moved_group(group, member):
    along = (group // DEPTH) * DEPTH + (group + 1) % DEPTH
    return jnp.where(member < 5, group, jnp.where(member < 7, along, (group + 1) % GROUPS))


def home_group(group, member):
    along = (group // DEPTH) * DEPTH + (group + DEPTH - 1) % DEPTH
    far = (group + GROUPS - 1) % GROUPS
    return jnp.where(member < 5, group, jnp.where(member < 7, along, far))


def pack_body(grp, mem, ghosts_hbm, slot_hbm, near_hbm, part_hbm, out, count, ghosts, slot, near, part, sem):
    copies = [
        pltpu.make_async_copy(source, target, sem.at[k])
        for k, (source, target) in enumerate(
            [(ghosts_hbm, ghosts), (slot_hbm, slot), (near_hbm, near), (part_hbm, part)]
        )
    ]
    for copy in copies:
        copy.start()
    out[...] = jnp.zeros(out.shape, F32)
    for g in range(GROUPS):
        count[g] = 0
        out[g * ROWS + 16 : g * ROWS + 17, :] = jnp.full((1, TILE), -1.0, F32)
    lane = lax.broadcasted_iota(jnp.int32, (1, TILE), 1)
    m = mem[0]
    for copy in copies[:3]:
        copy.wait()
    place = place_of(near[...], ghosts[0, 0]).astype(F32)
    place = jnp.concatenate(
        [place[:, GMAX : GMAX + HALF], place[:, :GMAX], place[:, GMAX + HALF :]], axis=1
    )
    row = jnp.full((1, TILE), -1.0, F32)
    for n in range(NB):
        first = LIST + n * TD
        piece = jnp.concatenate([place[n : n + 1], jnp.zeros((1, TILE - TD), F32)], axis=1)
        row = jnp.where((lane >= first) & (lane < first + TD), pltpu.roll(piece, first, 1), row)
    out[pl.ds(moved_group(grp[0], m) * ROWS + 16, 1), :] = row
    copies[3].wait()
    for t in range(TD):
        s = slot[t]
        g = moved_group(s // (TD * 8), m)
        n = count[g]
        count[g] = n + 1
        base = g * ROWS
        for r in range(8):
            out[pl.ds(base + n * 8 + r, 1), :] = part[r : r + 1, t * TILE : (t + 1) * TILE]
        label = pl.ds(base + 16, 1)
        here = (lane >= n * TD) & (lane < n * TD + TD)
        out[label, :] = jnp.where(here, rank(s % TD).astype(F32), out[label, :])


def split3(x):
    hi = x.astype(BF16).astype(F32)
    rest = x - hi
    mid = rest.astype(BF16).astype(F32)
    return hi, mid, rest - mid


def send_parts(odd, values, first, second):
    n = values.shape[-2]
    tail = values[..., n - GMAX :, :]
    head = values[..., n - HALF : n - GMAX, :]
    first[...] = jnp.where(odd, head, tail)
    second[...] = jnp.where(odd, tail, head)


def extend(odd, values, first, second):
    left = jnp.where(odd, first, second)
    right = jnp.where(odd, second, first)
    return jnp.concatenate([values, left, right], axis=-2)


def unpack_body(grp, mem, got, arranged, first, second, table):
    groups = got.shape[0] // ROWS
    odd = mem[0] % 2 == 1
    lane = lax.broadcasted_iota(jnp.int32, (groups, TILE), 1).astype(F32)
    labels = got[pl.ds(16, groups, stride=ROWS), :]
    marks = [
        jnp.where(values == lane, 1.0, 0.0)
        for values in (labels, pltpu.roll(labels, TILE - TD, 1))
    ]
    marks.append(jnp.zeros((TILE - 2 * groups, TILE), F32))
    choose = jnp.concatenate(marks, axis=0).T[:TD, : 2 * groups].astype(BF16)
    for r in range(8):
        tiles = jnp.concatenate(
            [got[pl.ds(n * 8 + r, groups, stride=ROWS), :] for n in range(2)], axis=0
        )
        moved = sum(
            jnp.dot(choose, piece.astype(BF16), preferred_element_type=F32)
            for piece in split3(tiles)
        )
        arranged[r] = moved
    mine = pl.ds(home_group(grp[0], mem[0]) * ROWS + 16, 1)
    table[...] = got[mine, :].astype(jnp.int32)
    send_parts(odd, arranged[0:6], first, second)


def place_of(entry, left):
    j = entry - left
    return jnp.where(j < 0, j + TD + GMAX, jnp.where(j < TD, rank(j), j + GMAX))


def rank(tile):
    return jnp.where(tile < GMAX, tile + HALF, jnp.where(tile < GMAX + HALF, tile - GMAX, tile))


LISTED = [pltpu.SMEM((1, TILE), jnp.int32), pltpu.SemaphoreType.DMA]


def spread_columns(cols, fields, tiles, first):
    turned = jnp.concatenate(fields, axis=0).T
    for f in range(5):
        for t in range(tiles):
            at = f * tiles + t
            cols[f, first + t] = jnp.broadcast_to(turned[:, at : at + 1], (TILE, TILE))


def columns_body(arranged, cols):
    spread_columns(cols, [arranged[f] for f in range(5)], TD, 0)


def density_edge(
    mem, table, arranged, first, second, held, dens, ext, dist, out1, out2, cols, near, sem
):
    listed = start_list(table, near, sem)
    odd = mem[0] % 2 == 1
    whole = extend(odd, arranged[0:6], first[...], second[...])
    ext[...] = whole
    spread_columns(cols, [whole[f, TD:] for f in range(5)], 2 * GMAX, TD)
    listed.wait()
    send_parts(odd, find_density(HALF, near, arranged, cols, dens, dist), out1, out2)


def density_inner(table, arranged, cols, dens, dist, near, sem):
    start_list(table, near, sem).wait()
    find_density(0, near, arranged, cols, dens, dist)


def find_density(begin, near, arranged, cols, dens, dist):
    def tile(k, carry):
        s = begin + k
        own = [arranged[f, pl.ds(s, 1), :] for f in range(5)]
        x_i, y_i, z_i, _, h_i = [jnp.broadcast_to(v, (CHUNK, TILE)) for v in own]
        pace = 2.0 / h_i
        total = jnp.zeros((CHUNK, TILE), F32)
        for n in range(NB):
            t = near[0, LIST + n * TD + s]
            for c in range(TILE // CHUNK):
                rows = pl.ds(c * CHUNK, CHUNK)
                dx = cols[0, t, rows, :] - x_i
                dy = cols[1, t, rows, :] - y_i
                dz = cols[2, t, rows, :] - z_i
                r2 = dx * dx + dy * dy + dz * dz
                r = r2 * lax.rsqrt(jnp.maximum(r2, 1e-30))
                dist[k, pl.ds(n * TILE + c * CHUNK, CHUNK), :] = r
                u = jnp.maximum(4.0 - r * pace, 0.0)
                u2 = u * u
                total = total + (cols[3, t, rows, :] * (5.0 - u)) * (u2 * u2)
        dens[pl.ds(k, 1), :] = jnp.sum(total, axis=0, keepdims=True)
        return carry

    lax.fori_loop(0, HALF, tile, 0)
    h = arranged[4, begin : begin + HALF]
    density = (KERNEL_NORM / 256.0) * dens[...] / (h * h * h)
    dens[...] = density
    return density


def forces_body(begin, table, arranged, cols, dist, *refs):
    *_, forces, near, sem = refs
    start_list(table, near, sem).wait()

    def tile(k, carry):
        s = begin + k
        h_i = jnp.broadcast_to(arranged[4, pl.ds(s, 1), :], (CHUNK, TILE))
        for n in range(NB):
            t = near[0, LIST + n * TD + s]
            for c in range(TILE // CHUNK):
                at = pl.ds(n * TILE + c * CHUNK, CHUNK)
                reach = cols[4, t, pl.ds(c * CHUNK, CHUNK), :] + h_i
                w = jnp.maximum(reach - dist[k, at, :], 0.0)
                p2 = reach * reach
                q = w / (p2 * p2)
                force = q * q * w
                high = force.astype(BF16)
                forces[k, 0, at, :] = high
                forces[k, 1, at, :] = (force - high.astype(F32)).astype(BF16)
        return carry

    lax.fori_loop(0, HALF, tile, 0)


def prepare(vectors, staged, operand):
    count = len(vectors)
    height = operand.shape[1]
    pieces = [split3(v) for v in vectors]
    for k in range(3):
        for q in range(count):
            staged[pl.ds(k * count + q, EXT, stride=height), :] = pieces[q][k]
    for t in range(EXT):
        operand[t] = staged[t * height : (t + 1) * height, :].astype(BF16)


def weigh(listed, near, forces, operand, result, count, tiles):
    height = operand.shape[1]
    listed.wait()
    for k, s in enumerate(tiles):
        row = jnp.concatenate([operand[near[0, LIST + n * TD + s]] for n in range(NB)], axis=1)
        block = forces[k // HALF] if isinstance(forces, tuple) else forces
        both = jnp.concatenate([block[k % HALF, 0], block[k % HALF, 1]], axis=1)
        got = jnp.dot(row, both, preferred_element_type=F32)
        result[k * height : (k + 1) * height, :] = got[:, TILE:] + got[:, :TILE]
    sums = []
    for q in range(count):
        parts = [result[pl.ds(k * count + q, len(tiles), stride=height), :] for k in (2, 1, 0)]
        sums.append(parts[0] + parts[1] + parts[2])
    return sums


def start_list(table, near, sem):
    listed = pltpu.make_async_copy(table, near, sem)
    listed.start()
    return listed


def limit(got, base, x, e, kappa, rho):
    square = jnp.zeros(e.shape, F32)
    for f in range(3):
        grad = (got[1 + f] - x[f] * got[0]) - e * (base[1 + f] - x[f] * base[0])
        square = square + grad * grad
    thick = kappa * rho
    ratio = jnp.sqrt(square) / (thick * e)
    return (2.0 + ratio) / ((6.0 + 3.0 * ratio + ratio * ratio) * thick)


INNER = range(HALF)
EDGE = range(HALF, TD)


def limiter_part(tiles, begin, listed, near, arranged, ext, forces, rho, e, fixed, operand, result, diff, sums):
    rows = slice(tiles[0], tiles[-1] + 1)
    got = weigh(listed, near, forces, operand, result, 8 if begin else 4, tiles)
    if begin:
        for q in range(4):
            fixed[q] = got[4 + q]
    base = [fixed[q] for q in range(4)]
    x = [ext[f, rows] - 0.5 for f in range(3)]
    value = limit(got, base, x, e[rows], arranged[6, rows], rho[rows])
    diff[...] = value
    sums[0] = base[0]
    sums[1] = got[0]
    return value


def limiter_edge(begin, *refs):
    *refs, staged, result, near, sem = refs
    listed = start_list(refs[1], near, sem)
    if begin:
        (mem, _, arranged, ext, forces, dens_inner, dens, d1, d2) = refs[:9]
        (diff, out1, out2, sums, operand, fixed, dens_ext) = refs[9:]
        odd = mem[0] % 2 == 1
        rho = extend(odd, jnp.concatenate([dens_inner[...], dens[...]], axis=0), d1[...], d2[...])
        dens_ext[...] = rho
        e = ext[5]
    else:
        (mem, _, arranged, ext, forces, dens_ext, fixed, e_inner, e_edge, e1, e2) = refs[:11]
        (diff, out1, out2, sums, operand, e_ext) = refs[11:]
        odd = mem[0] % 2 == 1
        rho = dens_ext[...]
        e = extend(odd, jnp.concatenate([e_inner[...], e_edge[...]], axis=0), e1[...], e2[...])
        e_ext[...] = e
    v = (160.0 * KERNEL_NORM) * ext[3] / rho
    x = [ext[f] - 0.5 for f in range(3)]
    ve = v * e
    vectors = [ve] + [ve * x[f] for f in range(3)]
    if begin:
        vectors = vectors + [v] + [v * x[f] for f in range(3)]
    prepare(vectors, staged, operand)
    value = limiter_part(
        EDGE, begin, listed, near, arranged, ext, forces, rho, e, fixed, operand, result, diff, sums
    )
    send_parts(odd, value, out1, out2)


def limiter_inner(begin, *refs):
    *refs, result, near, sem = refs
    listed = start_list(refs[0], near, sem)
    (_, arranged, ext, forces, rho, e_ext, operand) = refs[:7]
    if begin:
        diff, sums, fixed = refs[7:]
        e = e_ext[5]
    else:
        fixed, diff, sums = refs[7:]
        e = e_ext[...]
    limiter_part(
        INNER, begin, listed, near, arranged, ext, forces, rho, e, fixed, operand, result, diff, sums
    )


def step_energy(arranged, rows, rho, sums, own, got):
    scale = TIME_STEP / rho[rows]
    rate = scale * (own * sums[0] + got[0])
    inflow = scale * (own * sums[1] + got[1])
    return (arranged[5, rows] + TIME_STEP * arranged[7, rows] + inflow) / (1.0 + rate)


def jacobi_edge(last, *refs):
    *refs, staged, result, near, sem = refs
    listed = start_list(refs[1], near, sem)
    (mem, _, arranged, ext, forces, rho, e_ext, inner_sums, sums, inner, edge, d1, d2) = refs[:13]
    odd = mem[0] % 2 == 1
    own = jnp.concatenate([inner[...], edge[...]], axis=0)
    spread = extend(odd, own, d1[...], d2[...])
    vd = ((160.0 * KERNEL_NORM) * ext[3] / rho[...]) * spread
    e = e_ext[5] if len(e_ext.shape) == 3 else e_ext[...]
    if last:
        inner_forces, done, operand = refs[13:]
    else:
        new, out1, out2, operand = refs[13:]
    prepare([vd, vd * e], staged, operand)
    if last:
        got = weigh(listed, near, (inner_forces, forces), operand, result, 2, range(TD))
        both = [jnp.concatenate([inner_sums[q], sums[q]], axis=0) for q in range(2)]
        value = step_energy(arranged, slice(0, TD), rho, both, own, got)
        for k, v in enumerate((value, rho[:TD])):
            done[k * TD : k * TD + GMAX] = v[HALF : HALF + GMAX]
            done[k * TD + GMAX : k * TD + GMAX + HALF] = v[:HALF]
            done[k * TD + GMAX + HALF : (k + 1) * TD] = v[HALF + GMAX :]
    else:
        got = weigh(listed, near, forces, operand, result, 2, EDGE)
        value = step_energy(arranged, slice(HALF, TD), rho, sums, edge[...], got)
        new[...] = value
        send_parts(odd, value, out1, out2)


def jacobi_inner(table, arranged, forces, rho, operand, sums, inner, new, result, near, sem):
    listed = start_list(table, near, sem)
    got = weigh(listed, near, forces, operand, result, 2, INNER)
    new[...] = step_energy(arranged, slice(0, HALF), rho, sums, inner[...], got)


def workspace(height, tiles, staged):
    stage = [pltpu.VMEM((EXT * height, TILE), F32)] if staged else []
    return stage + [pltpu.VMEM((tiles * height, TILE), F32), *LISTED]


def swap(first, second):
    odd = [(owner(s), owner(s + 1)) for s in range(1, GROUPS * 8 - 1, 2)]
    even = [(owner(s), owner(s + 1)) for s in range(0, GROUPS * 8 - 1, 2)]
    got = []
    for value, pairs in ((first, even), (second, odd)):
        got.append(lax.ppermute(value, AXES, pairs + [(b, a) for a, b in pairs]))
    return got


def local(particles, new_slot, neighbours, ghosts):
    grp, mem = [lax.axis_index(axis).astype(jnp.int32).reshape(1) for axis in AXES]
    hbm = pl.BlockSpec(memory_space=pltpu.MemorySpace.HBM)
    outgoing = pl.pallas_call(
        pack_body,
        out_shape=jax.ShapeDtypeStruct((GROUPS * ROWS, TILE), F32),
        in_specs=[
            pl.BlockSpec(memory_space=SMEM),
            pl.BlockSpec(memory_space=SMEM),
            hbm,
            hbm,
            hbm,
            hbm,
        ],
        out_specs=pl.BlockSpec(memory_space=VMEM),
        scratch_shapes=[
            pltpu.SMEM((GROUPS,), jnp.int32),
            pltpu.SMEM((1, 2), jnp.int32),
            pltpu.SMEM((TD,), jnp.int32),
            pltpu.VMEM((NB, TD), jnp.int32),
            pltpu.VMEM((8, TD * TILE), F32),
            pltpu.SemaphoreType.DMA((4,)),
        ],
        name="pack",
        compiler_params=pltpu.CompilerParams(vmem_limit_bytes=VMEM_LIMIT),
    )(
        grp,
        mem,
        *(
            pltpu.with_memory_space_constraint(a, pltpu.MemorySpace.HBM)
            for a in (ghosts, new_slot, neighbours.T, particles)
        ),
    )
    received = lax.all_to_all(
        outgoing.reshape(GROUPS * ROWS, 1, TILE), "group", split_axis=0, concat_axis=0, tiled=True
    )
    edge = ((GMAX, TILE), F32)
    own = ((TD, TILE), F32)
    wide = ((EXT, TILE), F32)
    arranged, s1, s2, near = call(
        unpack_body,
        [
            ((8, TD, TILE), F32),
            ((6, GMAX, TILE), F32),
            ((6, GMAX, TILE), F32),
            ((1, TILE), jnp.int32),
        ],
        [],
        "unpack",
        grp,
        mem,
        received.reshape(GROUPS * ROWS, TILE),
    )
    table = (mem, near)
    s1, s2 = swap(s1, s2)
    (cols,) = call(columns_body, [((5, EXT, TILE, TILE), F32)], [], "columns", arranged)
    half = ((HALF, TILE), F32)
    apart = ((HALF, NB * TILE, TILE), F32)
    block = ((HALF, 2, NB * TILE, TILE), BF16)
    dens, ext, dist, r1, r2, cols = call(
        density_edge,
        [half, ((6, EXT, TILE), F32), apart, edge, edge, ((5, EXT, TILE, TILE), F32)],
        LISTED,
        "density_edge",
        *table,
        arranged,
        s1,
        s2,
        cols,
        alias={5: 5},
    )
    r1, r2 = swap(r1, r2)
    dens_inner, inner_dist = call(
        density_inner, [half, apart], LISTED, "density_inner", near, arranged, cols
    )
    (forces,) = call(
        lambda *refs: forces_body(HALF, *refs),
        [block],
        LISTED,
        "forces_edge",
        near,
        arranged,
        cols,
        dist,
    )
    shared = (*table, arranged, ext, forces)
    pair = ((2, HALF, TILE), F32)
    four = ((4, HALF, TILE), F32)
    for step in range(SWEEPS):
        begin = step == 0
        height = 24 if begin else 16
        operand = ((EXT, height, TILE), BF16)
        if begin:
            diff, d1, d2, sums, rows, fixed, dens_ext = call(
                lambda *refs: limiter_edge(True, *refs),
                [half, edge, edge, pair, operand, four, wide],
                workspace(height, HALF, True),
                "limiter_first_edge",
                *shared,
                dens_inner,
                dens,
                r1,
                r2,
            )
            e_ext = ext
        else:
            diff, d1, d2, sums, rows, e_ext = call(
                lambda *refs: limiter_edge(False, *refs),
                [half, edge, edge, pair, operand, wide],
                workspace(height, HALF, True),
                "limiter_edge",
                *shared,
                dens_ext,
                fixed,
                e_inner,
                e_edge,
                e1,
                e2,
            )
        d1, d2 = swap(d1, d2)
        if begin:
            (inner_forces,) = call(
                lambda *refs: forces_body(0, *refs),
                [block],
                LISTED,
                "forces_inner",
                near,
                arranged,
                cols,
                inner_dist,
                diff,
            )
        results = call(
            lambda *refs: limiter_inner(begin, *refs),
            [half, pair, four] if begin else [half, pair],
            workspace(height, HALF, False),
            "limiter_first_inner" if begin else "limiter_inner",
            near,
            arranged,
            ext,
            inner_forces,
            dens_ext,
            e_ext,
            rows,
            *(() if begin else (inner_fixed,)),
        )
        if begin:
            inner_diff, inner_sums, inner_fixed = results
        else:
            inner_diff, inner_sums = results
        last = step == SWEEPS - 1
        operand = ((EXT, 8, TILE), BF16)
        results = call(
            lambda *refs: jacobi_edge(last, *refs),
            [((2 * TD, TILE), F32)] if last else [half, edge, edge, operand],
            ([pltpu.VMEM(*operand)] if last else []) + workspace(8, TD if last else HALF, True),
            "jacobi_last" if last else "jacobi_edge",
            *shared,
            dens_ext,
            e_ext,
            inner_sums,
            sums,
            inner_diff,
            diff,
            d1,
            d2,
            *((inner_forces,) if last else ()),
        )
        if last:
            done = results[0]
        else:
            e_edge, e1, e2, rows = results
            e1, e2 = swap(e1, e2)
            (e_inner,) = call(
                jacobi_inner,
                [half],
                workspace(8, HALF, False),
                "jacobi_inner",
                near,
                arranged,
                inner_forces,
                dens_ext,
                rows,
                inner_sums,
                inner_diff,
            )
    done = lax.ppermute(done, AXES, [(owner(s), s) for s in range(GROUPS * 8)])
    return (done[:TD].reshape(-1), done[TD:].reshape(-1))


def solution(mesh):
    in_specs = (
        P(None, ("group", "member")),
        P(("group", "member")),
        P(("group", "member"), None),
        P(("group", "member"), None),
    )
    out_specs = (P(("group", "member")), P(("group", "member")))
    return jax.shard_map(local, mesh=mesh, in_specs=in_specs, out_specs=out_specs, check_vma=False)
```
